128 devices in a mesh: kpt: 4 (over x, y), gx: 32 (over z, core).
Axes of the slice: x: 2, y: 2, z: 16, core: 2. Of those that a mesh axis runs over, the one named last changes fastest.
The devices are a block of a 8x8x16 slice.
Arguments:
- e_field: float32 [2, 3, 256, 512, 128], P(None, None, ('kpt', 'gx')), parts along dimension 2, may hold values from -6 to 6
- h_field: float32 [2, 3, 256, 512, 128], P(None, None, ('kpt', 'gx')), parts along dimension 2, may hold values from -6 to 6
- labels: int32 [256, 512, 128], P(('kpt', 'gx')), parts along dimension 0, may hold values from 0 to 3
- kpoint: int32 [8], P('kpt'), parts along dimension 0, may hold values from 0 to 15
- eps_inf: float32 [4], replicated, may hold values from 1 to 12
- delta_eps: float32 [4], replicated, may hold values from 0.5 to 4
- omega_zero: float32 [4], replicated, may hold values from 0.2 to 1
- damping: float32 [4], replicated, may hold values from 0.05 to 0.8
Outputs:
- e_final: float32 [2, 3, 256, 512, 128], P(None, None, ('kpt', 'gx')), parts along dimension 2
- h_final: float32 [2, 3, 256, 512, 128], P(None, None, ('kpt', 'gx')), parts along dimension 2
The draws below stay inside these ranges and needn't reach their ends.
There are 4 independent parts, one for each index of `kpt`. The reference program is written for one: setup_inputs(seed, part) draws one part's arguments, and reference() takes and returns one part's arrays. A program takes and returns all parts, laid end to end along the dimension named above; an argument that names none is the same for every part. Nothing has to cross between parts.
Inputs may be any that keep to these rules, and one draw needn't show every extreme that they name: `kpoint`: entry 0 indexes the k-point along x, entry 1 along y, out of 16 each.
All inputs are finite; a program needn't handle non-finite values.
Results may differ from the reference program's by a relative error of at most 0.00002.
Values sent between devices are 32-bit elements; how exact they have to be, the bound alone decides.
A program may use at most 128 MiB of HBM per device.

```python
import math
import jax
import jax.numpy as jnp
from jax import lax

NY = 512
NZ = 128
ITERS = 12
LABELS = 4
KGRID = 16
NX = 64


def with_ends(entries, key, least, top_value):
    spot = [jax.random.randint(jax.random.fold_in(key, axis), (), 0, length) for axis, length in enumerate(entries.shape)]
    longest = entries.shape.index(max(entries.shape))
    beside = spot[:longest] + [(spot[longest] + 1) % entries.shape[longest]] + spot[longest + 1:]
    return entries.at[tuple(spot)].set(least).at[tuple(beside)].set(top_value)


def level_of(key, shape, split, smallest, largest):
    def one(dim, parts):
        draws = jax.random.uniform(jax.random.fold_in(jax.random.fold_in(key, 6), dim), (parts,), jnp.float32, smallest / len(split), largest / len(split))
        return jnp.repeat(jnp.exp(draws), shape[dim] // parts).reshape((-1,) + (1,) * (len(shape) - dim - 1))

    factor_of = one(*split[0])
    for cut in split[1:]:
        factor_of = factor_of * one(*cut)
    return factor_of


def noise(stream_key, shape, scale, bound, split=(), held_as=jnp.bfloat16):
    array = jax.random.normal(stream_key, shape, jnp.float32) * scale
    if len(split) > 0:
        array = level_of(stream_key, shape, split, -0.22, 0.18) * array
    return jnp.clip(array, min=-bound, max=bound).astype(held_as)


def setup_inputs(seed: int = 0, part: int = 0) -> dict:
    key_of = jax.random.split(jax.random.key(seed), 9)
    part_splits = jax.random.split(jax.random.fold_in(key_of[8], part), 9)
    return {
        "e_field": noise(part_splits[0], (2, 3, NX, NY, NZ), 1.0, 6.0, ((2, 32),), jnp.float32),
        "h_field": noise(part_splits[1], (2, 3, NX, NY, NZ), 1.0, 6.0, ((2, 32),), jnp.float32),
        "labels": with_ends(jax.random.randint(part_splits[2], (NX, NY, NZ), 0, LABELS), jax.random.fold_in(part_splits[2], 1), 0, LABELS - 1).astype(jnp.int32),
        "kpoint": jax.random.randint(part_splits[3], (2,), 0, KGRID).astype(jnp.int32),
        "eps_inf": jnp.clip(jnp.exp(jax.random.uniform(key_of[4], (LABELS,), jnp.float32, math.log(1.0), math.log(12.0))), 1.0, 12.0),
        "delta_eps": jnp.clip(jnp.exp(jax.random.uniform(key_of[5], (LABELS,), jnp.float32, math.log(0.5), math.log(4.0))), 0.5, 4.0),
        "omega_zero": jnp.clip(jnp.exp(jax.random.uniform(key_of[6], (LABELS,), jnp.float32, math.log(0.2), math.log(1.0))), 0.2, 1.0),
        "damping": jnp.clip(jnp.exp(jax.random.uniform(key_of[7], (LABELS,), jnp.float32, math.log(0.05), math.log(0.8))), 0.05, 0.8),
    }


time_step = 0.5


def cmul(field, cosv, sinv):
    return jnp.stack([field[0] * cosv - field[1] * sinv, field[0] * sinv + field[1] * cosv])


def next_axis(field, axis, cosv, sinv):
    rolled = jnp.roll(field, -1, axis=axis)
    count = field.shape[axis]
    inner = lax.slice_in_dim(rolled, 0, count - 1, axis=axis)
    last = cmul(lax.slice_in_dim(rolled, count - 1, count, axis=axis), cosv, sinv)
    return jnp.concatenate([inner, last], axis=axis)


def prev_axis(field, axis, cosv, sinv):
    rolled = jnp.roll(field, 1, axis=axis)
    count = field.shape[axis]
    first = cmul(lax.slice_in_dim(rolled, 0, 1, axis=axis), cosv, -sinv)
    inner = lax.slice_in_dim(rolled, 1, count, axis=axis)
    return jnp.concatenate([first, inner], axis=axis)


def next_z(field):
    zeros = jnp.zeros(field.shape[:-1] + (1,), jnp.float32)
    return jnp.concatenate([field[..., 1:], zeros], axis=-1)


def prev_z(field):
    zeros = jnp.zeros(field.shape[:-1] + (1,), jnp.float32)
    return jnp.concatenate([zeros, field[..., :-1]], axis=-1)


def per_cell(labels, table):
    picked = jnp.zeros(labels.shape, jnp.float32)
    for label in range(table.shape[0]):
        picked = picked + jnp.where(labels == label, table[label], jnp.float32(0.0))
    return picked


def reference(e_field, h_field, labels, kpoint, eps_inf, delta_eps, omega_zero, damping):
    theta_x = jnp.float32(2.0 * math.pi) * kpoint[0].astype(jnp.float32) / KGRID
    theta_y = jnp.float32(2.0 * math.pi) * kpoint[1].astype(jnp.float32) / KGRID
    cos_x, sin_x = jnp.cos(theta_x), jnp.sin(theta_x)
    cos_y, sin_y = jnp.cos(theta_y), jnp.sin(theta_y)
    half = damping * time_step / 2.0
    ce = per_cell(labels, time_step / eps_inf)
    ja = per_cell(labels, (1.0 - half) / (1.0 + half))
    jb = per_cell(labels, time_step * omega_zero * omega_zero / (1.0 + half))
    de = per_cell(labels, delta_eps)

    def advance(step, carry):
        efield, hfield, polar, current = carry
        ex, ey, ez = efield[:, 0], efield[:, 1], efield[:, 2]
        curl_x = (next_axis(ez, -2, cos_y, sin_y) - ez) - (next_z(ey) - ey)
        curl_y = (next_z(ex) - ex) - (next_axis(ez, -3, cos_x, sin_x) - ez)
        curl_z = (next_axis(ey, -3, cos_x, sin_x) - ey) - (next_axis(ex, -2, cos_y, sin_y) - ex)
        hfield = hfield - time_step * jnp.stack([curl_x, curl_y, curl_z], axis=1)
        hx, hy, hz = hfield[:, 0], hfield[:, 1], hfield[:, 2]
        kurl_x = (hz - prev_axis(hz, -2, cos_y, sin_y)) - (hy - prev_z(hy))
        kurl_y = (hx - prev_z(hx)) - (hz - prev_axis(hz, -3, cos_x, sin_x))
        kurl_z = (hy - prev_axis(hy, -3, cos_x, sin_x)) - (hx - prev_axis(hx, -2, cos_y, sin_y))
        kurl = jnp.stack([kurl_x, kurl_y, kurl_z], axis=1)
        current = ja * current + jb * (de * efield - polar)
        polar = polar + time_step * current
        efield = efield + ce * (kurl - current)
        return efield, hfield, polar, current

    zeros = jnp.zeros(e_field.shape, jnp.float32)
    efield, hfield, polar, current = lax.fori_loop(0, ITERS, advance, (e_field, h_field, zeros, zeros))
    return efield, hfield
```

```python
import functools
import math

import jax
import jax.numpy as jnp
from jax import lax
from jax.experimental import pallas as pl
from jax.experimental.pallas import tpu as pltpu
from jax.sharding import PartitionSpec as P

MESH = pl.DeviceIdType.MESH
ITERS = 12
KGRID = 16
DT = 0.5
CHUNKS = 8
LAG = 4
BLOCK = 16
PAD = 8


def next_z(field, last):
    return jnp.where(last, 0.0, pltpu.roll(field, field.shape[1] - 1, 1))


def prev_z(field, first):
    return jnp.where(first, 0.0, pltpu.roll(field, 1, 1))


def kernel(
    e_in, h_in, labels_in, kpoint, eps_inf, delta_eps, omega_zero, damping,
    e_out, h_out,
    e, h, p, cur, ce, ja, jb, de, labels, ge, gh, phase,
    load_e, load_h, load_l, send_e, recv_e, send_h, recv_h, store_e, store_h,
):
    planes, ny, nz = labels.shape
    rows = ny // CHUNKS
    last_plane = planes - 1
    size = lax.axis_size("gx")
    me = lax.axis_index("gx")
    right = lax.rem(me + 1, size)
    left = lax.rem(me + size - 1, size)

    def span(c, pad=0):
        return pl.ds(pl.multiple_of(c * rows + pad, 8), rows)

    def get_e(c):
        return pltpu.make_async_copy(
            e_in.at[:, :, :, span(c)], e.at[:, :, :, span(c)], load_e.at[c])

    def get_h(c):
        return pltpu.make_async_copy(
            h_in.at[:, :, :, span(c)], h.at[:, :, :, span(c, PAD)], load_h.at[c])

    def get_labels():
        return pltpu.make_async_copy(labels_in, labels, load_l)

    def put_e(c):
        return pltpu.make_async_copy(
            e.at[:, :, :, span(c)], e_out.at[:, :, :, span(c)], store_e.at[c])

    def put_h(c):
        return pltpu.make_async_copy(
            h.at[:, :, :, span(c, PAD)], h_out.at[:, :, :, span(c)], store_h.at[c])

    def ship_e(c, source):
        return pltpu.make_async_remote_copy(
            src_ref=source.at[:, 1:3, 0, span(c)], dst_ref=ge.at[:, :, span(c)],
            send_sem=send_e.at[c], recv_sem=recv_e.at[c],
            device_id={"gx": left}, device_id_type=MESH)

    def ship_h(c):
        return pltpu.make_async_remote_copy(
            src_ref=h.at[:, 1:3, last_plane, span(c, PAD)], dst_ref=gh.at[:, :, span(c)],
            send_sem=send_h.at[c], recv_sem=recv_h.at[c],
            device_id={"gx": right}, device_id_type=MESH)

    barrier = pltpu.get_barrier_semaphore()
    for neighbour in (left, right):
        pl.semaphore_signal(barrier, inc=1, device_id={"gx": neighbour}, device_id_type=MESH)
    for c in range(CHUNKS):
        get_e(c).start()
        get_h(c).start()
        if c == 0:
            get_labels().start()
    pl.semaphore_wait(barrier, 2)
    for c in range(CHUNKS):
        ship_e(c, e_in).start()

    tile = (8, nz)
    turn = jnp.float32(2.0 * math.pi)
    theta_x = turn * jnp.full(tile, kpoint[0], jnp.int32).astype(jnp.float32) / KGRID
    theta_y = turn * jnp.full(tile, kpoint[1], jnp.int32).astype(jnp.float32) / KGRID
    cos_x, sin_x = jnp.cos(theta_x), jnp.sin(theta_x)
    phase[0] = jnp.where(me == size - 1, cos_x, 1.0)
    phase[1] = jnp.where(me == size - 1, sin_x, 0.0)
    phase[2] = jnp.where(me == 0, cos_x, 1.0)
    phase[3] = jnp.where(me == 0, -sin_x, 0.0)
    phase[4] = jnp.cos(theta_y)
    phase[5] = jnp.sin(theta_y)

    shape = (BLOCK, nz)

    def whole(value):
        return jnp.full(shape, value, jnp.float32)

    tables = []
    for label in range(eps_inf.shape[0]):
        half = whole(damping[label]) * (DT / 2.0)
        omega = whole(omega_zero[label])
        tables.append((
            DT / whole(eps_inf[label]),
            (1.0 - half) / (1.0 + half),
            DT * omega * omega / (1.0 + half),
            whole(delta_eps[label]),
        ))
    for which in range(4):
        for label in range(len(tables)):
            phase[8 + 4 * which + label] = tables[label][which][:8]

    def clear(block, carry):
        at = pl.ds(pl.multiple_of(block * BLOCK, 8), BLOCK)
        zero = jnp.zeros(shape, jnp.float32)
        for q in range(2):
            for comp in range(3):
                for x in range(planes):
                    p[q, comp, x, at] = zero
                    cur[q, comp, x, at] = zero
        return carry

    lax.fori_loop(0, ny // BLOCK, clear, 0)

    def spread(row):
        return jnp.concatenate([phase[row]] * (BLOCK // 8), axis=0)

    get_labels().wait()

    def media(block, carry):
        at = pl.ds(pl.multiple_of(block * BLOCK, 8), BLOCK)
        for x in range(planes):
            label = labels[x, at]
            for which, dst in enumerate((ce, ja, jb, de)):
                picked = spread(8 + 4 * which)
                for k in range(1, len(tables)):
                    picked = jnp.where(label == k, spread(8 + 4 * which + k), picked)
                dst[x, at] = picked
        return carry

    lax.fori_loop(0, ny // BLOCK, media, 0)

    column = lax.broadcasted_iota(jnp.int32, shape, 1)
    is_first, is_last = column == 0, column == nz - 1

    def wrap_e():
        cy, sy = phase[4][0:1], phase[5][0:1]
        for comp in (0, 2):
            for x in range(planes):
                re, im = e[0, comp, x, 0:1], e[1, comp, x, 0:1]
                e[0, comp, x, ny:ny + 1] = re * cy - im * sy
                e[1, comp, x, ny:ny + 1] = re * sy + im * cy

    def wrap_h():
        cy, sy = phase[4][0:1], phase[5][0:1]
        bottom = PAD + ny - 1
        for comp in (0, 2):
            for x in range(planes):
                re, im = h[0, comp, x, bottom:bottom + 1], h[1, comp, x, bottom:bottom + 1]
                h[0, comp, x, PAD - 1:PAD] = re * cy + im * sy
                h[1, comp, x, PAD - 1:PAD] = im * cy - re * sy

    def turned(ghost, at, row):
        cx, sx = spread(row), spread(row + 1)
        out = []
        for comp in range(2):
            re, im = ghost[0, comp, at], ghost[1, comp, at]
            out.append((re * cx - im * sx, re * sx + im * cx))
        return out

    def magnetic(c):
        def block(b, carry):
            y = c * rows + b * BLOCK
            at = pl.ds(pl.multiple_of(y, 8), BLOCK)
            up = pl.ds(y + 1, BLOCK)
            ath = pl.ds(pl.multiple_of(y + PAD, 8), BLOCK)
            far = turned(ge, at, 0)
            for q in range(2):
                for x in range(planes):
                    ex, ey, ez = e[q, 0, x, at], e[q, 1, x, at], e[q, 2, x, at]
                    if x == last_plane:
                        ey_x, ez_x = far[0][q], far[1][q]
                    else:
                        ey_x, ez_x = e[q, 1, x + 1, at], e[q, 2, x + 1, at]
                    ex_y, ez_y = e[q, 0, x, up], e[q, 2, x, up]
                    ex_z, ey_z = next_z(ex, is_last), next_z(ey, is_last)
                    h[q, 0, x, ath] -= DT * ((ez_y - ez) - (ey_z - ey))
                    h[q, 1, x, ath] -= DT * ((ex_z - ex) - (ez_x - ez))
                    h[q, 2, x, ath] -= DT * ((ey_x - ey) - (ex_y - ex))
            return carry

        lax.fori_loop(0, rows // BLOCK, block, 0)

    def electric(c):
        def block(b, carry):
            y = c * rows + b * BLOCK
            at = pl.ds(pl.multiple_of(y, 8), BLOCK)
            ath = pl.ds(pl.multiple_of(y + PAD, 8), BLOCK)
            down = pl.ds(y + PAD - 1, BLOCK)
            far = turned(gh, at, 2)
            for x in range(planes):
                c_e, j_a, j_b, d_e = ce[x, at], ja[x, at], jb[x, at], de[x, at]
                for q in range(2):
                    hx, hy, hz = h[q, 0, x, ath], h[q, 1, x, ath], h[q, 2, x, ath]
                    if x == 0:
                        hy_x, hz_x = far[0][q], far[1][q]
                    else:
                        hy_x, hz_x = h[q, 1, x - 1, ath], h[q, 2, x - 1, ath]
                    hx_y, hz_y = h[q, 0, x, down], h[q, 2, x, down]
                    hx_z, hy_z = prev_z(hx, is_first), prev_z(hy, is_first)
                    curls = (
                        (hz - hz_y) - (hy - hy_z),
                        (hx - hx_z) - (hz - hz_x),
                        (hy - hy_x) - (hx - hx_y),
                    )
                    for comp, curl in enumerate(curls):
                        field, polar = e[q, comp, x, at], p[q, comp, x, at]
                        current = j_a * cur[q, comp, x, at] + j_b * (d_e * field - polar)
                        cur[q, comp, x, at] = current
                        p[q, comp, x, at] = polar + DT * current
                        e[q, comp, x, at] = field + c_e * (curl - current)
            return carry

        lax.fori_loop(0, rows // BLOCK, block, 0)

    total = ITERS * CHUNKS
    get_e(0).wait()
    wrap_e()

    def advance(i, carry):
        @pl.when(i < total)
        def _():
            n, j = i // CHUNKS, i % CHUNKS
            c = (n + j) % CHUNKS

            @pl.when(n == 0)
            def _():
                @pl.when(j + 1 < CHUNKS)
                def _():
                    get_e(j + 1).wait()

                get_h(j).wait()

            @pl.when(n > 0)
            def _():
                ship_h(c).wait_send()

            ship_e(c, e).wait_recv()
            magnetic(c)

            @pl.when(c == CHUNKS - 1)
            def _():
                wrap_h()

            ship_h(c).start()

            @pl.when(n == ITERS - 1)
            def _():
                put_h(c).start()

        @pl.when(i >= LAG)
        def _():
            n, j = (i - LAG) // CHUNKS, (i - LAG) % CHUNKS
            c = (n + 1 + j) % CHUNKS
            ship_h(c).wait_recv()
            ship_e(c, e).wait_send()
            electric(c)

            @pl.when(c == 0)
            def _():
                wrap_e()

            @pl.when(n < ITERS - 1)
            def _():
                ship_e(c, e).start()

            @pl.when(n == ITERS - 1)
            def _():
                put_e(c).start()

        return carry

    lax.fori_loop(0, total + LAG, advance, 0)
    for c in range(CHUNKS):
        ship_h(c).wait_send()
        put_h(c).wait()
        put_e(c).wait()


def shards(e_field, h_field, labels, kpoint, eps_inf, delta_eps, omega_zero, damping):
    planes, ny, nz = labels.shape
    fields = (2, 3, planes)
    anywhere = pl.BlockSpec(memory_space=pl.ANY)
    scalars = pl.BlockSpec(memory_space=pltpu.SMEM)

    def vmem(*shape):
        return pltpu.VMEM(shape, jnp.float32)

    def many():
        return pltpu.SemaphoreType.DMA((CHUNKS,))

    return pl.pallas_call(
        kernel,
        out_shape=(
            jax.ShapeDtypeStruct(e_field.shape, jnp.float32),
            jax.ShapeDtypeStruct(h_field.shape, jnp.float32),
        ),
        in_specs=[anywhere] * 3 + [scalars] * 5,
        out_specs=(anywhere, anywhere),
        scratch_shapes=[
            vmem(*fields, ny + PAD, nz),
            vmem(*fields, ny + PAD, nz),
            vmem(*fields, ny, nz),
            vmem(*fields, ny, nz),
            vmem(planes, ny, nz),
            vmem(planes, ny, nz),
            vmem(planes, ny, nz),
            vmem(planes, ny, nz),
            pltpu.VMEM((planes, ny, nz), jnp.int32),
            vmem(2, 2, ny, nz),
            vmem(2, 2, ny, nz),
            vmem(24, 8, nz),
            many(), many(), pltpu.SemaphoreType.DMA,
            many(), many(), many(), many(), many(), many(),
        ],
        compiler_params=pltpu.CompilerParams(
            collective_id=0, has_side_effects=True, vmem_limit_bytes=60 * 1024 * 1024,
        ),
    )(e_field, h_field, labels, kpoint, eps_inf, delta_eps, omega_zero, damping)


def solution(mesh):
    placed = (
        P(None, None, ("kpt", "gx"), None, None),
        P(None, None, ("kpt", "gx"), None, None),
        P(("kpt", "gx"), None, None),
        P("kpt"),
        P(),
        P(),
        P(),
        P(),
    )
    return jax.shard_map(
        shards,
        mesh=mesh,
        in_specs=placed,
        out_specs=(
            P(None, None, ("kpt", "gx"), None, None),
            P(None, None, ("kpt", "gx"), None, None),
        ),
        check_vma=False,
    )
```

```python
import functools
import math

import jax
import jax.numpy as jnp
from jax import lax
from jax.experimental import pallas as pl
from jax.experimental.pallas import tpu as pltpu
from jax.sharding import PartitionSpec as P

MESH = pl.DeviceIdType.MESH
ITERS = 12
KGRID = 16
DT = 0.5
CHUNKS = 16
AHEAD = 8
BLOCK = 16
PAD = 8
KERNEL_VMEM = 57 * 1024 * 1024


def next_z(field, last):
    return jnp.where(last, 0.0, pltpu.roll(field, field.shape[1] - 1, 1))


def prev_z(field, first):
    return jnp.where(first, 0.0, pltpu.roll(field, 1, 1))


def kernel(
    e_in, h_in, labels_in, kpoint, eps_inf, delta_eps, omega_zero, damping,
    e, h,
    p, cur, ce, ja, jb, de, labels, part, ge, ga, phase,
    load_e, load_h, load_l, send_e, recv_e, send_a, recv_a,
):
    planes, ny, nz = labels.shape
    rows = ny // CHUNKS
    last_plane = planes - 1
    size = lax.axis_size("gx")
    me = lax.axis_index("gx")
    right = lax.rem(me + 1, size)
    left = lax.rem(me + size - 1, size)

    def span(c, pad=0):
        return pl.ds(pl.multiple_of(c * rows + pad, 8), rows)

    def get_e(c):
        return pltpu.make_async_copy(
            e_in.at[:, :, :, span(c)], e.at[:, :, :, span(c)], load_e.at[c])

    def get_h(c):
        return pltpu.make_async_copy(
            h_in.at[:, :, :, span(c)], h.at[:, :, :, span(c, PAD)], load_h.at[c])

    def get_labels():
        return pltpu.make_async_copy(labels_in, labels, load_l)

    def ship_e(n, c, source):
        return pltpu.make_async_remote_copy(
            src_ref=source.at[:, 1:3, 0, span(c)], dst_ref=ge.at[n % 2, :, :, span(c)],
            send_sem=send_e.at[c], recv_sem=recv_e.at[n % 2, c],
            device_id={"gx": left}, device_id_type=MESH)

    def ship_a(n, c):
        return pltpu.make_async_remote_copy(
            src_ref=part.at[:, :, span(c)], dst_ref=ga.at[n % 2, :, :, span(c)],
            send_sem=send_a.at[c], recv_sem=recv_a.at[n % 2, c],
            device_id={"gx": right}, device_id_type=MESH)

    barrier = pltpu.get_barrier_semaphore()
    for neighbour in (left, right):
        pl.semaphore_signal(barrier, inc=1, device_id={"gx": neighbour}, device_id_type=MESH)
    get_e(0).start()
    for c in range(CHUNKS):
        if c + 1 < CHUNKS:
            get_e(c + 1).start()
        get_h(c).start()
    get_labels().start()
    pl.semaphore_wait(barrier, 2)
    for c in range(CHUNKS):
        ship_e(0, c, e_in).start()

    tile = (8, nz)
    turn = jnp.float32(2.0 * math.pi)
    theta_x = turn * jnp.full(tile, kpoint[0], jnp.int32).astype(jnp.float32) / KGRID
    theta_y = turn * jnp.full(tile, kpoint[1], jnp.int32).astype(jnp.float32) / KGRID
    cos_x, sin_x = jnp.cos(theta_x), jnp.sin(theta_x)
    phase[0] = jnp.where(me == size - 1, cos_x, 1.0)
    phase[1] = jnp.where(me == size - 1, sin_x, 0.0)
    phase[2] = jnp.where(me == 0, cos_x, 1.0)
    phase[3] = jnp.where(me == 0, -sin_x, 0.0)
    phase[4] = jnp.cos(theta_y)
    phase[5] = jnp.sin(theta_y)

    def whole(value):
        return jnp.full(tile, value, jnp.float32)

    count = eps_inf.shape[0]
    for label in range(count):
        half = whole(damping[label]) * (DT / 2.0)
        omega = whole(omega_zero[label])
        phase[8 + label] = DT / whole(eps_inf[label])
        phase[8 + count + label] = (1.0 - half) / (1.0 + half)
        phase[8 + 2 * count + label] = DT * omega * omega / (1.0 + half)
        phase[8 + 3 * count + label] = whole(delta_eps[label])

    shape = (BLOCK, nz)

    def spread(row):
        return jnp.concatenate([phase[row]] * (BLOCK // 8), axis=0)

    def media(block, carry):
        at = pl.ds(pl.multiple_of(block * BLOCK, 8), BLOCK)
        zero = jnp.zeros(shape, jnp.float32)
        for x in range(planes):
            label = labels[x, at]
            for which, dst in enumerate((ce, ja, jb, de)):
                picked = spread(8 + count * which)
                for k in range(1, count):
                    picked = jnp.where(label == k, spread(8 + count * which + k), picked)
                dst[x, at] = picked
            for q in range(2):
                for comp in range(3):
                    p[q, comp, x, at] = zero
                    cur[q, comp, x, at] = zero
        return carry

    column = lax.broadcasted_iota(jnp.int32, shape, 1)
    is_first, is_last = column == 0, column == nz - 1

    def wrap_e():
        cy, sy = phase[4][0:1], phase[5][0:1]
        for comp in (0, 2):
            for x in range(planes):
                re, im = e[0, comp, x, 0:1], e[1, comp, x, 0:1]
                e[0, comp, x, ny:ny + 1] = re * cy - im * sy
                e[1, comp, x, ny:ny + 1] = re * sy + im * cy

    def wrap_h():
        cy, sy = phase[4][0:1], phase[5][0:1]
        bottom = PAD + ny - 1
        for comp in (0, 2):
            for x in range(planes):
                re, im = h[0, comp, x, bottom:bottom + 1], h[1, comp, x, bottom:bottom + 1]
                h[0, comp, x, PAD - 1:PAD] = re * cy + im * sy
                h[1, comp, x, PAD - 1:PAD] = im * cy - re * sy

    def turned(ghost, slot, at, row):
        cx, sx = spread(row), spread(row + 1)
        out = []
        for comp in range(2):
            re, im = ghost[slot, 0, comp, at], ghost[slot, 1, comp, at]
            out.append((re * cx - im * sx, re * sx + im * cx))
        return out

    def magnetic(c):
        def block(b, carry):
            y = c * rows + b * BLOCK
            at = pl.ds(pl.multiple_of(y, 8), BLOCK)
            up = pl.ds(y + 1, BLOCK)
            ath = pl.ds(pl.multiple_of(y + PAD, 8), BLOCK)
            for q in range(2):
                for x in range(planes):
                    ex, ey, ez = e[q, 0, x, at], e[q, 1, x, at], e[q, 2, x, at]
                    ex_y, ez_y = e[q, 0, x, up], e[q, 2, x, up]
                    ex_z, ey_z = next_z(ex, is_last), next_z(ey, is_last)
                    h[q, 0, x, ath] -= DT * ((ez_y - ez) - (ey_z - ey))
                    if x == last_plane:
                        hy = h[q, 1, x, ath] - DT * ((ex_z - ex) + ez)
                        hz = h[q, 2, x, ath] + DT * (ey + (ex_y - ex))
                        part[q, 0, at] = hy
                        part[q, 1, at] = hz
                        h[q, 1, x, ath] = hy
                        h[q, 2, x, ath] = hz
                    else:
                        ey_x, ez_x = e[q, 1, x + 1, at], e[q, 2, x + 1, at]
                        h[q, 1, x, ath] -= DT * ((ex_z - ex) - (ez_x - ez))
                        h[q, 2, x, ath] -= DT * ((ey_x - ey) - (ex_y - ex))
            return carry

        lax.fori_loop(0, rows // BLOCK, block, 0)

    def complete(slot, c):
        def block(b, carry):
            y = c * rows + b * BLOCK
            at = pl.ds(pl.multiple_of(y, 8), BLOCK)
            ath = pl.ds(pl.multiple_of(y + PAD, 8), BLOCK)
            far_y, far_z = turned(ge, slot, at, 0)
            for q in range(2):
                h[q, 1, last_plane, ath] += DT * far_z[q]
                h[q, 2, last_plane, ath] -= DT * far_y[q]
            return carry

        lax.fori_loop(0, rows // BLOCK, block, 0)

    def electric(slot, c):
        def block(b, carry):
            y = c * rows + b * BLOCK
            at = pl.ds(pl.multiple_of(y, 8), BLOCK)
            ath = pl.ds(pl.multiple_of(y + PAD, 8), BLOCK)
            down = pl.ds(y + PAD - 1, BLOCK)
            far = turned(ga, slot, at, 2)
            for x in range(planes):
                c_e, j_a, j_b, d_e = ce[x, at], ja[x, at], jb[x, at], de[x, at]
                for q in range(2):
                    fields = [e[q, comp, x, at] for comp in range(3)]
                    hx, hy, hz = h[q, 0, x, ath], h[q, 1, x, ath], h[q, 2, x, ath]
                    if x == 0:
                        hy_x = far[0][q] + DT * fields[2]
                        hz_x = far[1][q] - DT * fields[1]
                    else:
                        hy_x, hz_x = h[q, 1, x - 1, ath], h[q, 2, x - 1, ath]
                    hx_y, hz_y = h[q, 0, x, down], h[q, 2, x, down]
                    hx_z, hy_z = prev_z(hx, is_first), prev_z(hy, is_first)
                    curls = (
                        (hz - hz_y) - (hy - hy_z),
                        (hx - hx_z) - (hz - hz_x),
                        (hy - hy_x) - (hx - hx_y),
                    )
                    for comp, curl in enumerate(curls):
                        field, polar = fields[comp], p[q, comp, x, at]
                        current = j_a * cur[q, comp, x, at] + j_b * (d_e * field - polar)
                        cur[q, comp, x, at] = current
                        p[q, comp, x, at] = polar + DT * current
                        e[q, comp, x, at] = field + c_e * (curl - current)
            return carry

        lax.fori_loop(0, rows // BLOCK, block, 0)

    total = ITERS * CHUNKS

    def send_part(n, c):
        magnetic(c)
        ship_a(n, c).start()

    get_e(0).wait()
    wrap_e()

    def first(j, carry):
        get_e(j + 1).wait()
        get_h(j).wait()
        send_part(0, j)
        return carry

    lax.fori_loop(0, AHEAD, first, 0)
    get_labels().wait()
    lax.fori_loop(0, ny // BLOCK, media, 0)

    def advance(i, carry):
        @pl.when(i < total)
        def _():
            n, j = i // CHUNKS, i % CHUNKS
            c = (n + j) % CHUNKS
            ship_e(n, c, e).wait_recv()
            complete(n % 2, c)

            @pl.when(c == CHUNKS - 1)
            def _():
                wrap_h()

        @pl.when(i > 0)
        def _():
            n, j = (i - 1) // CHUNKS, (i - 1) % CHUNKS
            c = (n + 1 + j) % CHUNKS
            ship_a(n, c).wait_recv()
            ship_e(n, c, e).wait_send()
            electric(n % 2, c)

            @pl.when(c == 0)
            def _():
                wrap_e()

            @pl.when(n < ITERS - 1)
            def _():
                ship_e(n + 1, c, e).start()

        @pl.when(i + AHEAD < total)
        def _():
            n, j = (i + AHEAD) // CHUNKS, (i + AHEAD) % CHUNKS
            c = (n + j) % CHUNKS

            @pl.when(n == 0)
            def _():
                @pl.when(j + 1 < CHUNKS)
                def _():
                    get_e(j + 1).wait()

                get_h(j).wait()

            @pl.when(n > 0)
            def _():
                ship_a(n, c).wait_send()

            send_part(n, c)

        return carry

    lax.fori_loop(0, total + 1, advance, 0)
    for c in range(CHUNKS):
        ship_a(ITERS - 1, c).wait_send()


def deliver(e, h, e_out, h_out, sems):
    ny = e_out.shape[3]
    copies = []
    for q in range(2):
        for comp in range(3):
            copies.append(pltpu.make_async_copy(
                e.at[q, comp, :, 0:ny], e_out.at[q, comp], sems.at[0, q, comp]))
            copies.append(pltpu.make_async_copy(
                h.at[q, comp, :, PAD:PAD + ny], h_out.at[q, comp], sems.at[1, q, comp]))
    for copy in copies:
        copy.start()
    for copy in copies:
        copy.wait()


def shards(e_field, h_field, labels, kpoint, eps_inf, delta_eps, omega_zero, damping):
    planes, ny, nz = labels.shape
    fields = (2, 3, planes)
    anywhere = pl.BlockSpec(memory_space=pltpu.HBM)
    scalars = pl.BlockSpec(memory_space=pltpu.SMEM)
    near = pl.BlockSpec(memory_space=pltpu.VMEM)

    def vmem(*shape):
        return pltpu.VMEM(shape, jnp.float32)

    def many(*lead):
        return pltpu.SemaphoreType.DMA(lead + (CHUNKS,))

    e_last, h_last = pl.pallas_call(
        kernel,
        out_shape=(vmem(*fields, ny + PAD, nz), vmem(*fields, ny + PAD, nz)),
        in_specs=[anywhere] * 3 + [scalars] * 5,
        out_specs=(near, near),
        scratch_shapes=[
            vmem(*fields, ny, nz),
            vmem(*fields, ny, nz),
            vmem(planes, ny, nz),
            vmem(planes, ny, nz),
            vmem(planes, ny, nz),
            vmem(planes, ny, nz),
            pltpu.VMEM((planes, ny, nz), jnp.int32),
            vmem(2, 2, ny, nz),
            vmem(2, 2, 2, ny, nz),
            vmem(2, 2, 2, ny, nz),
            vmem(24, 8, nz),
            many(), many(), pltpu.SemaphoreType.DMA,
            many(), many(2), many(), many(2),
        ],
        compiler_params=pltpu.CompilerParams(
            collective_id=0, has_side_effects=True, vmem_limit_bytes=KERNEL_VMEM,
        ),
    )(e_field, h_field, labels, kpoint, eps_inf, delta_eps, omega_zero, damping)
    return pl.pallas_call(
        deliver,
        out_shape=(
            jax.ShapeDtypeStruct(e_field.shape, jnp.float32),
            jax.ShapeDtypeStruct(h_field.shape, jnp.float32),
        ),
        in_specs=[near, near],
        out_specs=(anywhere, anywhere),
        scratch_shapes=[pltpu.SemaphoreType.DMA((2, 2, 3))],
        compiler_params=pltpu.CompilerParams(vmem_limit_bytes=1024 * 1024),
    )(e_last, h_last)


def solution(mesh):
    placed = (
        P(None, None, ("kpt", "gx"), None, None),
        P(None, None, ("kpt", "gx"), None, None),
        P(("kpt", "gx"), None, None),
        P("kpt"),
        P(),
        P(),
        P(),
        P(),
    )
    return jax.shard_map(
        shards,
        mesh=mesh,
        in_specs=placed,
        out_specs=(
            P(None, None, ("kpt", "gx"), None, None),
            P(None, None, ("kpt", "gx"), None, None),
        ),
        check_vma=False,
    )
```

```python
import functools
import math

import jax
import jax.numpy as jnp
from jax import lax
from jax.experimental import pallas as pl
from jax.experimental.pallas import tpu as pltpu
from jax.sharding import PartitionSpec as P

MESH = pl.DeviceIdType.MESH
ITERS = 12
KGRID = 16
DT = 0.5
CHUNKS = 16
AHEAD = 12
BLOCK = 32
PIECES = 1
PAD = 8
KERNEL_VMEM = 57 * 1024 * 1024


def next_z(field, last):
    return jnp.where(last, 0.0, pltpu.roll(field, field.shape[1] - 1, 1))


def prev_z(field, first):
    return jnp.where(first, 0.0, pltpu.roll(field, 1, 1))


def kernel(
    e_in, h_in, labels_in, kpoint_in, eps_inf_in, delta_eps_in, omega_zero_in, damping_in,
    e, h,
    kpoint, eps_inf, delta_eps, omega_zero, damping, load_s,
    p, cur, ce, ja, jb, de, labels, part, ge, ga, phase,
    load_e, load_h, load_l, send_e, recv_e, send_a, recv_a,
):
    planes, ny, nz = labels.shape
    count = eps_inf.shape[0]
    rows = ny // CHUNKS
    last_plane = planes - 1
    size = lax.axis_size("gx")
    me = lax.axis_index("gx")
    right = lax.rem(me + 1, size)
    left = lax.rem(me + size - 1, size)

    def span(c, pad=0):
        return pl.ds(pl.multiple_of(c * rows + pad, 8), rows)

    starts = [0] + [k for k in (2, 4, 8, 16, 32) if k < CHUNKS]
    groups = list(zip(starts, starts[1:] + [CHUNKS]))

    def get_e(g):
        low, high = groups[g]
        at = pl.ds(low * rows, (high - low) * rows)
        return pltpu.make_async_copy(
            e_in.at[:, :, :, at], e.at[:, :, :, at], load_e.at[g])

    def get_h(g):
        low, high = groups[g]
        at = pl.ds(low * rows, (high - low) * rows)
        ath = pl.ds(low * rows + PAD, (high - low) * rows)
        return pltpu.make_async_copy(
            h_in.at[:, :, :, at], h.at[:, :, :, ath], load_h.at[g])

    def get_labels():
        return pltpu.make_async_copy(labels_in, labels, load_l)

    def ship_e(n, c):
        return pltpu.make_async_remote_copy(
            src_ref=e.at[:, 1:3, 0, span(c)], dst_ref=ge.at[n % 2, :, :, span(c)],
            send_sem=send_e.at[c], recv_sem=recv_e.at[n % 2, c],
            device_id={"gx": left}, device_id_type=MESH)

    def ship_a(n, c):
        return pltpu.make_async_remote_copy(
            src_ref=part.at[:, :, span(c)], dst_ref=ga.at[n % 2, :, :, span(c)],
            send_sem=send_a.at[c], recv_sem=recv_a.at[n % 2, c],
            device_id={"gx": right}, device_id_type=MESH)

    barrier = pltpu.get_barrier_semaphore()
    for neighbour in (left, right):
        pl.semaphore_signal(barrier, inc=1, device_id={"gx": neighbour}, device_id_type=MESH)
    for g in range(len(groups)):
        get_e(g).start()
        get_h(g).start()
    get_labels().start()
    scalars = [
        pltpu.make_async_copy(source, target, load_s.at[k])
        for k, (source, target) in enumerate((
            (kpoint_in, kpoint), (eps_inf_in, eps_inf), (delta_eps_in, delta_eps),
            (omega_zero_in, omega_zero), (damping_in, damping)))
    ]
    for copy in scalars:
        copy.start()

    shape = (BLOCK, nz)

    def prepare():
        tile = (8, nz)
        turn = jnp.float32(2.0 * math.pi)
        theta_x = turn * jnp.full(tile, kpoint[0], jnp.int32).astype(jnp.float32) / KGRID
        theta_y = turn * jnp.full(tile, kpoint[1], jnp.int32).astype(jnp.float32) / KGRID
        cos_x, sin_x = jnp.cos(theta_x), jnp.sin(theta_x)
        phase[0] = jnp.where(me == size - 1, cos_x, 1.0)
        phase[1] = jnp.where(me == size - 1, sin_x, 0.0)
        phase[2] = jnp.where(me == 0, cos_x, 1.0)
        phase[3] = jnp.where(me == 0, -sin_x, 0.0)
        phase[4] = jnp.cos(theta_y)
        phase[5] = jnp.sin(theta_y)

        def whole(value):
            return jnp.full(tile, value, jnp.float32)

        for label in range(count):
            half = whole(damping[label]) * (DT / 2.0)
            omega = whole(omega_zero[label])
            phase[8 + label] = DT / whole(eps_inf[label])
            phase[8 + count + label] = (1.0 - half) / (1.0 + half)
            phase[8 + 2 * count + label] = DT * omega * omega / (1.0 + half)
            phase[8 + 3 * count + label] = whole(delta_eps[label])

    def spread(row):
        return jnp.concatenate([phase[row]] * (BLOCK // 8), axis=0)

    def media(block, carry):
        at = pl.ds(pl.multiple_of(block * BLOCK, 8), BLOCK)
        zero = jnp.zeros(shape, jnp.float32)
        for x in range(planes):
            label = labels[x, at]
            for which, dst in enumerate((ce, ja, jb, de)):
                picked = spread(8 + count * which)
                for k in range(1, count):
                    picked = jnp.where(label == k, spread(8 + count * which + k), picked)
                dst[x, at] = picked
            for q in range(2):
                for comp in range(3):
                    p[q, comp, x, at] = zero
                    cur[q, comp, x, at] = zero
        return carry

    column = lax.broadcasted_iota(jnp.int32, shape, 1)
    is_first, is_last = column == 0, column == nz - 1

    def wrap_e():
        cy, sy = phase[4][0:1], phase[5][0:1]
        for comp in (0, 2):
            for x in range(planes):
                re, im = e[0, comp, x, 0:1], e[1, comp, x, 0:1]
                e[0, comp, x, ny:ny + 1] = re * cy - im * sy
                e[1, comp, x, ny:ny + 1] = re * sy + im * cy

    def wrap_h():
        cy, sy = phase[4][0:1], phase[5][0:1]
        bottom = PAD + ny - 1
        for comp in (0, 2):
            for x in range(planes):
                re, im = h[0, comp, x, bottom:bottom + 1], h[1, comp, x, bottom:bottom + 1]
                h[0, comp, x, PAD - 1:PAD] = re * cy + im * sy
                h[1, comp, x, PAD - 1:PAD] = im * cy - re * sy

    def turned(ghost, slot, at, row):
        cx, sx = spread(row), spread(row + 1)
        out = []
        for comp in range(2):
            re, im = ghost[slot, 0, comp, at], ghost[slot, 1, comp, at]
            out.append((re * cx - im * sx, re * sx + im * cx))
        return out

    def magnetic(c):
        def block(b, carry):
            y = c * rows + b * BLOCK
            at = pl.ds(pl.multiple_of(y, 8), BLOCK)
            up = pl.ds(y + 1, BLOCK)
            ath = pl.ds(pl.multiple_of(y + PAD, 8), BLOCK)
            for q in range(2):
                for x in range(planes):
                    ex, ey, ez = e[q, 0, x, at], e[q, 1, x, at], e[q, 2, x, at]
                    ex_y, ez_y = e[q, 0, x, up], e[q, 2, x, up]
                    ex_z, ey_z = next_z(ex, is_last), next_z(ey, is_last)
                    h[q, 0, x, ath] -= DT * ((ez_y - ez) - (ey_z - ey))
                    if x == last_plane:
                        hy = h[q, 1, x, ath] - DT * ((ex_z - ex) + ez)
                        hz = h[q, 2, x, ath] + DT * (ey + (ex_y - ex))
                        part[q, 0, at] = hy
                        part[q, 1, at] = hz
                        h[q, 1, x, ath] = hy
                        h[q, 2, x, ath] = hz
                    else:
                        ey_x, ez_x = e[q, 1, x + 1, at], e[q, 2, x + 1, at]
                        h[q, 1, x, ath] -= DT * ((ex_z - ex) - (ez_x - ez))
                        h[q, 2, x, ath] -= DT * ((ey_x - ey) - (ex_y - ex))
            return carry

        lax.fori_loop(0, rows // BLOCK, block, 0)

    def complete(slot, c):
        def block(b, carry):
            y = c * rows + b * BLOCK
            at = pl.ds(pl.multiple_of(y, 8), BLOCK)
            ath = pl.ds(pl.multiple_of(y + PAD, 8), BLOCK)
            far_y, far_z = turned(ge, slot, at, 0)
            for q in range(2):
                h[q, 1, last_plane, ath] += DT * far_z[q]
                h[q, 2, last_plane, ath] -= DT * far_y[q]
            return carry

        lax.fori_loop(0, rows // BLOCK, block, 0)

    def electric(slot, c):
        def block(b, carry):
            y = c * rows + b * BLOCK
            at = pl.ds(pl.multiple_of(y, 8), BLOCK)
            ath = pl.ds(pl.multiple_of(y + PAD, 8), BLOCK)
            down = pl.ds(y + PAD - 1, BLOCK)
            far = turned(ga, slot, at, 2)
            for x in range(planes):
                c_e, j_a, j_b, d_e = ce[x, at], ja[x, at], jb[x, at], de[x, at]
                for q in range(2):
                    fields = [e[q, comp, x, at] for comp in range(3)]
                    hx, hy, hz = h[q, 0, x, ath], h[q, 1, x, ath], h[q, 2, x, ath]
                    if x == 0:
                        hy_x = far[0][q] + DT * fields[2]
                        hz_x = far[1][q] - DT * fields[1]
                    else:
                        hy_x, hz_x = h[q, 1, x - 1, ath], h[q, 2, x - 1, ath]
                    hx_y, hz_y = h[q, 0, x, down], h[q, 2, x, down]
                    hx_z, hy_z = prev_z(hx, is_first), prev_z(hy, is_first)
                    curls = (
                        (hz - hz_y) - (hy - hy_z),
                        (hx - hx_z) - (hz - hz_x),
                        (hy - hy_x) - (hx - hx_y),
                    )
                    for comp, curl in enumerate(curls):
                        field, polar = fields[comp], p[q, comp, x, at]
                        current = j_a * cur[q, comp, x, at] + j_b * (d_e * field - polar)
                        cur[q, comp, x, at] = current
                        p[q, comp, x, at] = polar + DT * current
                        e[q, comp, x, at] = field + c_e * (curl - current)
            return carry

        lax.fori_loop(0, rows // BLOCK, block, 0)

    total = ITERS * CHUNKS
    pl.semaphore_wait(barrier, 2)

    def advance(step, carry):
        i = step - AHEAD

        @pl.when(i == 0)
        def _():
            for copy in scalars:
                copy.wait()
            prepare()
            wrap_e()
            get_labels().wait()
            lax.fori_loop(0, ny // BLOCK, media, 0)

        @pl.when((i >= 0) & (i < total))
        def _():
            n, j = i // CHUNKS, i % CHUNKS
            c = (n + j) % CHUNKS
            ship_e(n, c).wait_recv()
            complete(n % 2, c)

            @pl.when(c == CHUNKS - 1)
            def _():
                wrap_h()

        @pl.when(i > 0)
        def _():
            n, j = (i - 1) // CHUNKS, (i - 1) % CHUNKS
            c = (n + 1 + j) % CHUNKS
            ship_a(n, c).wait_recv()
            ship_e(n, c).wait_send()
            electric(n % 2, c)

            @pl.when(c == 0)
            def _():
                wrap_e()

            @pl.when(n < ITERS - 1)
            def _():
                ship_e(n + 1, c).start()

        @pl.when(step < total)
        def _():
            n, j = step // CHUNKS, step % CHUNKS
            c = (n + j) % CHUNKS

            for g, (low, high) in enumerate(groups):
                @pl.when(step == max(low - 1, 0))
                def _():
                    get_e(g).wait()
                    for chunk in range(low, high):
                        ship_e(0, chunk).start()
                    get_h(g).wait()

            @pl.when(n > 0)
            def _():
                ship_a(n, c).wait_send()

            magnetic(c)
            ship_a(n, c).start()

        return carry

    lax.fori_loop(0, total + 1 + AHEAD, advance, 0)
    for c in range(CHUNKS):
        ship_a(ITERS - 1, c).wait_send()


def deliver(e, h, e_out, h_out, sems):
    ny = e_out.shape[3]
    copies = []
    step = ny // PIECES
    for q in range(2):
        for comp in range(3):
            for k in range(PIECES):
                y = k * step
                copies.append(pltpu.make_async_copy(
                    e.at[q, comp, :, y:y + step], e_out.at[q, comp, :, y:y + step],
                    sems.at[0, q, comp, k]))
                copies.append(pltpu.make_async_copy(
                    h.at[q, comp, :, PAD + y:PAD + y + step], h_out.at[q, comp, :, y:y + step],
                    sems.at[1, q, comp, k]))
    for copy in copies:
        copy.start()
    for copy in copies:
        copy.wait()


def shards(e_field, h_field, labels, kpoint, eps_inf, delta_eps, omega_zero, damping):
    planes, ny, nz = labels.shape
    fields = (2, 3, planes)
    anywhere = pl.BlockSpec(memory_space=pltpu.HBM)
    near = pl.BlockSpec(memory_space=pltpu.VMEM)

    def vmem(*shape):
        return pltpu.VMEM(shape, jnp.float32)

    def many(*lead):
        return pltpu.SemaphoreType.DMA(lead + (CHUNKS,))

    e_last, h_last = pl.pallas_call(
        kernel,
        out_shape=(vmem(*fields, ny + PAD, nz), vmem(*fields, ny + PAD, nz)),
        in_specs=[anywhere] * 8,
        out_specs=(near, near),
        scratch_shapes=[
            pltpu.SMEM(kpoint.shape, jnp.int32),
            *(pltpu.SMEM(eps_inf.shape, jnp.float32) for _ in range(4)),
            pltpu.SemaphoreType.DMA((5,)),
            vmem(*fields, ny, nz),
            vmem(*fields, ny, nz),
            vmem(planes, ny, nz),
            vmem(planes, ny, nz),
            vmem(planes, ny, nz),
            vmem(planes, ny, nz),
            pltpu.VMEM((planes, ny, nz), jnp.int32),
            vmem(2, 2, ny, nz),
            vmem(2, 2, 2, ny, nz),
            vmem(2, 2, 2, ny, nz),
            vmem(24, 8, nz),
            many(), many(), pltpu.SemaphoreType.DMA,
            many(), many(2), many(), many(2),
        ],
        compiler_params=pltpu.CompilerParams(
            collective_id=0, has_side_effects=True, vmem_limit_bytes=KERNEL_VMEM,
        ),
    )(e_field, h_field, labels, kpoint, eps_inf, delta_eps, omega_zero, damping)
    return pl.pallas_call(
        deliver,
        out_shape=(
            jax.ShapeDtypeStruct(e_field.shape, jnp.float32),
            jax.ShapeDtypeStruct(h_field.shape, jnp.float32),
        ),
        in_specs=[near, near],
        out_specs=(anywhere, anywhere),
        scratch_shapes=[pltpu.SemaphoreType.DMA((2, 2, 3, PIECES))],
        compiler_params=pltpu.CompilerParams(vmem_limit_bytes=1024 * 1024),
    )(e_last, h_last)


def solution(mesh):
    placed = (
        P(None, None, ("kpt", "gx"), None, None),
        P(None, None, ("kpt", "gx"), None, None),
        P(("kpt", "gx"), None, None),
        P("kpt"),
        P(),
        P(),
        P(),
        P(),
    )
    return jax.shard_map(
        shards,
        mesh=mesh,
        in_specs=placed,
        out_specs=(
            P(None, None, ("kpt", "gx"), None, None),
            P(None, None, ("kpt", "gx"), None, None),
        ),
        check_vma=False,
    )
```

```python
import functools
import math

import jax
import jax.numpy as jnp
from jax import lax
from jax.experimental import pallas as pl
from jax.experimental.pallas import tpu as pltpu
from jax.sharding import PartitionSpec as P

MESH = pl.DeviceIdType.MESH
ITERS = 12
KGRID = 16
DT = 0.5
CHUNKS = 16
AHEAD = 14
VIA_FROM = 1
VIA_TO = 6
VIA_FIRST = 10
VIA_SECOND = 27
BLOCK = 32
PIECES = 1
PAD = 8
KERNEL_VMEM = 57 * 1024 * 1024


def next_z(field, last):
    return jnp.where(last, 0.0, pltpu.roll(field, field.shape[1] - 1, 1))


def prev_z(field, first):
    return jnp.where(first, 0.0, pltpu.roll(field, 1, 1))


def kernel(
    e_in, h_in, labels_in, kpoint_in, eps_inf_in, delta_eps_in, omega_zero_in, damping_in,
    e, h,
    kpoint, eps_inf, delta_eps, omega_zero, damping, load_s,
    p, cur, ce, ja, jb, de, labels, part, sent, ge, ga, phase,
    load_e, load_h, load_l, send_e, recv_e, send_a, recv_a,
    relay, send_r, recv_r,
):
    planes, ny, nz = labels.shape
    count = eps_inf.shape[0]
    rows = ny // CHUNKS
    last_plane = planes - 1
    size = lax.axis_size("gx")
    me = lax.axis_index("gx")
    right = lax.rem(me + 1, size)
    relay_one = 2 * size // 3
    relay_two = size // 3 + 1
    left = lax.rem(me + size - 1, size)

    def span(c, pad=0):
        return pl.ds(pl.multiple_of(c * rows + pad, 8), rows)

    starts = [0] + [k for k in (2, 4, 8, 16, 32) if k < CHUNKS]
    groups = list(zip(starts, starts[1:] + [CHUNKS]))

    def get_e(g):
        low, high = groups[g]
        at = pl.ds(low * rows, (high - low) * rows)
        return pltpu.make_async_copy(
            e_in.at[:, :, :, at], e.at[:, :, :, at], load_e.at[g])

    def get_h(g):
        low, high = groups[g]
        at = pl.ds(low * rows, (high - low) * rows)
        ath = pl.ds(low * rows + PAD, (high - low) * rows)
        return pltpu.make_async_copy(
            h_in.at[:, :, :, at], h.at[:, :, :, ath], load_h.at[g])

    def get_labels():
        return pltpu.make_async_copy(labels_in, labels, load_l)

    def ship_first(c):
        return pltpu.make_async_remote_copy(
            src_ref=e.at[:, 1:3, 0, span(c)], dst_ref=ge.at[0, :, :, span(c)],
            send_sem=send_e.at[0, c], recv_sem=recv_e.at[0, c],
            device_id={"gx": left}, device_id_type=MESH)

    def ship_e(n, c):
        return pltpu.make_async_remote_copy(
            src_ref=sent.at[n % 2, :, :, span(c)], dst_ref=ge.at[n % 2, :, :, span(c)],
            send_sem=send_e.at[n % 2, c], recv_sem=recv_e.at[n % 2, c],
            device_id={"gx": left}, device_id_type=MESH)

    def ship_a(n, c):
        return pltpu.make_async_remote_copy(
            src_ref=part.at[:, :, span(c)], dst_ref=ga.at[n % 2, :, :, span(c)],
            send_sem=send_a.at[c], recv_sem=recv_a.at[n % 2, c],
            device_id={"gx": right}, device_id_type=MESH)

    def ship_via(n, c):
        return pltpu.make_async_remote_copy(
            src_ref=part.at[:, :, span(c)], dst_ref=relay.at[n - VIA_FROM],
            send_sem=send_a.at[c], recv_sem=recv_r.at[n - VIA_FROM],
            device_id={"gx": relay_one}, device_id_type=MESH)

    def pass_on(n):
        return pltpu.make_async_remote_copy(
            src_ref=relay.at[n - VIA_FROM], dst_ref=relay.at[n - VIA_FROM],
            send_sem=send_r.at[n - VIA_FROM], recv_sem=recv_r.at[n - VIA_FROM],
            device_id={"gx": relay_two}, device_id_type=MESH)

    def pass_last(n):
        return pltpu.make_async_remote_copy(
            src_ref=relay.at[n - VIA_FROM], dst_ref=ga.at[n % 2, :, :, span(n % CHUNKS)],
            send_sem=send_r.at[n - VIA_FROM], recv_sem=recv_a.at[n % 2, n % CHUNKS],
            device_id={"gx": 0}, device_id_type=MESH)

    barrier = pltpu.get_barrier_semaphore()
    for neighbour in (left, right):
        pl.semaphore_signal(barrier, inc=1, device_id={"gx": neighbour}, device_id_type=MESH)
    for target, source in ((relay_one, size - 1), (relay_two, relay_one), (0, relay_two)):
        @pl.when(me == target)
        def _():
            pl.semaphore_signal(barrier, inc=1, device_id={"gx": source}, device_id_type=MESH)
    for g in range(len(groups)):
        get_e(g).start()
        get_h(g).start()
    get_labels().start()
    scalars = [
        pltpu.make_async_copy(source, target, load_s.at[k])
        for k, (source, target) in enumerate((
            (kpoint_in, kpoint), (eps_inf_in, eps_inf), (delta_eps_in, delta_eps),
            (omega_zero_in, omega_zero), (damping_in, damping)))
    ]
    for copy in scalars:
        copy.start()

    shape = (BLOCK, nz)

    def prepare():
        tile = (8, nz)
        turn = jnp.float32(2.0 * math.pi)
        theta_x = turn * jnp.full(tile, kpoint[0], jnp.int32).astype(jnp.float32) / KGRID
        theta_y = turn * jnp.full(tile, kpoint[1], jnp.int32).astype(jnp.float32) / KGRID
        cos_x, sin_x = jnp.cos(theta_x), jnp.sin(theta_x)
        phase[0] = jnp.where(me == size - 1, cos_x, 1.0)
        phase[1] = jnp.where(me == size - 1, sin_x, 0.0)
        phase[2] = jnp.where(me == 0, cos_x, 1.0)
        phase[3] = jnp.where(me == 0, -sin_x, 0.0)
        phase[4] = jnp.cos(theta_y)
        phase[5] = jnp.sin(theta_y)

        def whole(value):
            return jnp.full(tile, value, jnp.float32)

        for label in range(count):
            half = whole(damping[label]) * (DT / 2.0)
            omega = whole(omega_zero[label])
            phase[8 + label] = DT / whole(eps_inf[label])
            phase[8 + count + label] = (1.0 - half) / (1.0 + half)
            phase[8 + 2 * count + label] = DT * omega * omega / (1.0 + half)
            phase[8 + 3 * count + label] = whole(delta_eps[label])

    def spread(row):
        return jnp.concatenate([phase[row]] * (BLOCK // 8), axis=0)

    def media(block, carry):
        at = pl.ds(pl.multiple_of(block * BLOCK, 8), BLOCK)
        zero = jnp.zeros(shape, jnp.float32)
        for x in range(planes):
            label = labels[x, at]
            for which, dst in enumerate((ce, ja, jb, de)):
                picked = spread(8 + count * which)
                for k in range(1, count):
                    picked = jnp.where(label == k, spread(8 + count * which + k), picked)
                dst[x, at] = picked
            for q in range(2):
                for comp in range(3):
                    p[q, comp, x, at] = zero
                    cur[q, comp, x, at] = zero
        return carry

    column = lax.broadcasted_iota(jnp.int32, shape, 1)
    is_first, is_last = column == 0, column == nz - 1

    def wrap_e():
        cy, sy = phase[4][0:1], phase[5][0:1]
        for comp in (0, 2):
            for x in range(planes):
                re, im = e[0, comp, x, 0:1], e[1, comp, x, 0:1]
                e[0, comp, x, ny:ny + 1] = re * cy - im * sy
                e[1, comp, x, ny:ny + 1] = re * sy + im * cy

    def wrap_h():
        cy, sy = phase[4][0:1], phase[5][0:1]
        bottom = PAD + ny - 1
        for comp in (0, 2):
            for x in range(planes):
                re, im = h[0, comp, x, bottom:bottom + 1], h[1, comp, x, bottom:bottom + 1]
                h[0, comp, x, PAD - 1:PAD] = re * cy + im * sy
                h[1, comp, x, PAD - 1:PAD] = im * cy - re * sy

    def turned(ghost, slot, at, row):
        cx, sx = spread(row), spread(row + 1)
        out = []
        for comp in range(2):
            re, im = ghost[slot, 0, comp, at], ghost[slot, 1, comp, at]
            out.append((re * cx - im * sx, re * sx + im * cx))
        return out

    def magnetic(c):
        def block(b, carry):
            y = c * rows + b * BLOCK
            at = pl.ds(pl.multiple_of(y, 8), BLOCK)
            up = pl.ds(y + 1, BLOCK)
            ath = pl.ds(pl.multiple_of(y + PAD, 8), BLOCK)
            for q in range(2):
                for x in range(planes):
                    ex, ey, ez = e[q, 0, x, at], e[q, 1, x, at], e[q, 2, x, at]
                    ex_y, ez_y = e[q, 0, x, up], e[q, 2, x, up]
                    ex_z, ey_z = next_z(ex, is_last), next_z(ey, is_last)
                    h[q, 0, x, ath] -= DT * ((ez_y - ez) - (ey_z - ey))
                    if x == last_plane:
                        hy = h[q, 1, x, ath] - DT * ((ex_z - ex) + ez)
                        hz = h[q, 2, x, ath] + DT * (ey + (ex_y - ex))
                        part[q, 0, at] = hy
                        part[q, 1, at] = hz
                        h[q, 1, x, ath] = hy
                        h[q, 2, x, ath] = hz
                    else:
                        ey_x, ez_x = e[q, 1, x + 1, at], e[q, 2, x + 1, at]
                        h[q, 1, x, ath] -= DT * ((ex_z - ex) - (ez_x - ez))
                        h[q, 2, x, ath] -= DT * ((ey_x - ey) - (ex_y - ex))
            return carry

        lax.fori_loop(0, rows // BLOCK, block, 0)

    def complete(slot, c):
        def block(b, carry):
            y = c * rows + b * BLOCK
            at = pl.ds(pl.multiple_of(y, 8), BLOCK)
            ath = pl.ds(pl.multiple_of(y + PAD, 8), BLOCK)
            far_y, far_z = turned(ge, slot, at, 0)
            for q in range(2):
                h[q, 1, last_plane, ath] += DT * far_z[q]
                h[q, 2, last_plane, ath] -= DT * far_y[q]
            return carry

        lax.fori_loop(0, rows // BLOCK, block, 0)

    def electric(slot, c):
        def block(b, carry):
            y = c * rows + b * BLOCK
            at = pl.ds(pl.multiple_of(y, 8), BLOCK)
            ath = pl.ds(pl.multiple_of(y + PAD, 8), BLOCK)
            down = pl.ds(y + PAD - 1, BLOCK)
            far = turned(ga, slot, at, 2)
            for x in range(planes):
                c_e, j_a, j_b, d_e = ce[x, at], ja[x, at], jb[x, at], de[x, at]
                for q in range(2):
                    fields = [e[q, comp, x, at] for comp in range(3)]
                    hx, hy, hz = h[q, 0, x, ath], h[q, 1, x, ath], h[q, 2, x, ath]
                    if x == 0:
                        hy_x = far[0][q] + DT * fields[2]
                        hz_x = far[1][q] - DT * fields[1]
                    else:
                        hy_x, hz_x = h[q, 1, x - 1, ath], h[q, 2, x - 1, ath]
                    hx_y, hz_y = h[q, 0, x, down], h[q, 2, x, down]
                    hx_z, hy_z = prev_z(hx, is_first), prev_z(hy, is_first)
                    curls = (
                        (hz - hz_y) - (hy - hy_z),
                        (hx - hx_z) - (hz - hz_x),
                        (hy - hy_x) - (hx - hx_y),
                    )
                    for comp, curl in enumerate(curls):
                        field, polar = fields[comp], p[q, comp, x, at]
                        current = j_a * cur[q, comp, x, at] + j_b * (d_e * field - polar)
                        cur[q, comp, x, at] = current
                        p[q, comp, x, at] = polar + DT * current
                        field = field + c_e * (curl - current)
                        e[q, comp, x, at] = field
                        if x == 0 and comp > 0:
                            sent[1 - slot, q, comp - 1, at] = field
            return carry

        lax.fori_loop(0, rows // BLOCK, block, 0)

    total = ITERS * CHUNKS
    relays = (me == relay_one) | (me == relay_two)
    three = relays | (me == size - 1)

    @pl.when(three)
    def _():
        pl.semaphore_wait(barrier, 3)

    @pl.when(jnp.logical_not(three))
    def _():
        pl.semaphore_wait(barrier, 2)

    def advance(step, carry):
        i = step - AHEAD

        @pl.when(i == 0)
        def _():
            for copy in scalars:
                copy.wait()
            prepare()
            wrap_e()
            get_labels().wait()
            lax.fori_loop(0, ny // BLOCK, media, 0)

        @pl.when((i >= 0) & (i < total))
        def _():
            n, j = i // CHUNKS, i % CHUNKS
            c = (n + j) % CHUNKS
            ship_e(n, c).wait_recv()
            complete(n % 2, c)

            @pl.when(c == CHUNKS - 1)
            def _():
                wrap_h()

        @pl.when(i > 0)
        def _():
            n, j = (i - 1) // CHUNKS, (i - 1) % CHUNKS
            c = (n + 1 + j) % CHUNKS
            ship_a(n, c).wait_recv()

            @pl.when(n == 0)
            def _():
                ship_first(c).wait_send()

            @pl.when(n > 1)
            def _():
                ship_e(n - 1, c).wait_send()

            electric(n % 2, c)

            @pl.when(c == 0)
            def _():
                wrap_e()

            @pl.when(n < ITERS - 1)
            def _():
                ship_e(n + 1, c).start()

        @pl.when(step < total)
        def _():
            n, j = step // CHUNKS, step % CHUNKS
            c = (n + j) % CHUNKS

            for g, (low, high) in enumerate(groups):
                @pl.when(step == max(low - 1, 0))
                def _():
                    get_e(g).wait()
                    for chunk in range(low, high):
                        ship_first(chunk).start()
                    get_h(g).wait()

            @pl.when(n > 0)
            def _():
                ship_a(n, c).wait_send()

            magnetic(c)
            via = (me == size - 1) & (j == 0) & (n >= VIA_FROM) & (n < VIA_TO)

            @pl.when(via)
            def _():
                ship_via(n, c).start()

            @pl.when(jnp.logical_not(via))
            def _():
                ship_a(n, c).start()

        for relay_at, late, send in ((relay_one, VIA_FIRST, pass_on), (relay_two, VIA_SECOND, pass_last)):
            behind = step - late

            @pl.when((me == relay_at) & (behind >= VIA_FROM * CHUNKS)
                     & (behind < VIA_TO * CHUNKS) & (behind % CHUNKS == 0))
            def _():
                n = behind // CHUNKS
                pass_on(n).wait_recv()
                send(n).start()

        return carry

    lax.fori_loop(0, total + 1 + AHEAD, advance, 0)
    for c in range(CHUNKS):
        ship_a(ITERS - 1, c).wait_send()
        ship_e(ITERS - 1, c).wait_send()

    @pl.when(relays)
    def _():
        for n in range(VIA_FROM, VIA_TO):
            pass_on(n).wait_send()


def deliver(e, h, e_out, h_out, sems):
    ny = e_out.shape[3]
    copies = []
    step = ny // PIECES
    for q in range(2):
        for comp in range(3):
            for k in range(PIECES):
                y = k * step
                copies.append(pltpu.make_async_copy(
                    e.at[q, comp, :, y:y + step], e_out.at[q, comp, :, y:y + step],
                    sems.at[0, q, comp, k]))
                copies.append(pltpu.make_async_copy(
                    h.at[q, comp, :, PAD + y:PAD + y + step], h_out.at[q, comp, :, y:y + step],
                    sems.at[1, q, comp, k]))
    for copy in copies:
        copy.start()
    for copy in copies:
        copy.wait()


def shards(e_field, h_field, labels, kpoint, eps_inf, delta_eps, omega_zero, damping):
    planes, ny, nz = labels.shape
    fields = (2, 3, planes)
    anywhere = pl.BlockSpec(memory_space=pltpu.HBM)
    near = pl.BlockSpec(memory_space=pltpu.VMEM)

    def vmem(*shape):
        return pltpu.VMEM(shape, jnp.float32)

    def many(*lead):
        return pltpu.SemaphoreType.DMA(lead + (CHUNKS,))

    e_last, h_last = pl.pallas_call(
        kernel,
        out_shape=(vmem(*fields, ny + PAD, nz), vmem(*fields, ny + PAD, nz)),
        in_specs=[anywhere] * 8,
        out_specs=(near, near),
        scratch_shapes=[
            pltpu.SMEM(kpoint.shape, jnp.int32),
            *(pltpu.SMEM(eps_inf.shape, jnp.float32) for _ in range(4)),
            pltpu.SemaphoreType.DMA((5,)),
            vmem(*fields, ny, nz),
            vmem(*fields, ny, nz),
            vmem(planes, ny, nz),
            vmem(planes, ny, nz),
            vmem(planes, ny, nz),
            vmem(planes, ny, nz),
            pltpu.VMEM((planes, ny, nz), jnp.int32),
            vmem(2, 2, ny, nz),
            vmem(2, 2, 2, ny, nz),
            vmem(2, 2, 2, ny, nz),
            vmem(2, 2, 2, ny, nz),
            vmem(24, 8, nz),
            many(), many(), pltpu.SemaphoreType.DMA,
            many(2), many(2), many(), many(2),
            vmem(VIA_TO - VIA_FROM, 2, 2, ny // CHUNKS, nz),
            pltpu.SemaphoreType.DMA((VIA_TO - VIA_FROM,)),
            pltpu.SemaphoreType.DMA((VIA_TO - VIA_FROM,)),
        ],
        compiler_params=pltpu.CompilerParams(
            collective_id=0, has_side_effects=True, vmem_limit_bytes=KERNEL_VMEM,
        ),
    )(e_field, h_field, labels, kpoint, eps_inf, delta_eps, omega_zero, damping)
    return pl.pallas_call(
        deliver,
        out_shape=(
            jax.ShapeDtypeStruct(e_field.shape, jnp.float32),
            jax.ShapeDtypeStruct(h_field.shape, jnp.float32),
        ),
        in_specs=[near, near],
        out_specs=(anywhere, anywhere),
        scratch_shapes=[pltpu.SemaphoreType.DMA((2, 2, 3, PIECES))],
        compiler_params=pltpu.CompilerParams(vmem_limit_bytes=1024 * 1024),
    )(e_last, h_last)


def solution(mesh):
    placed = (
        P(None, None, ("kpt", "gx"), None, None),
        P(None, None, ("kpt", "gx"), None, None),
        P(("kpt", "gx"), None, None),
        P("kpt"),
        P(),
        P(),
        P(),
        P(),
    )
    return jax.shard_map(
        shards,
        mesh=mesh,
        in_specs=placed,
        out_specs=(
            P(None, None, ("kpt", "gx"), None, None),
            P(None, None, ("kpt", "gx"), None, None),
        ),
        check_vma=False,
    )
```

```python
import functools
import math

import jax
import jax.numpy as jnp
from jax import lax
from jax.experimental import pallas as pl
from jax.experimental.pallas import tpu as pltpu
from jax.sharding import PartitionSpec as P

MESH = pl.DeviceIdType.MESH
ITERS = 12
KGRID = 16
DT = 0.5
CHUNKS = 16
AHEAD = 14
VIA_FROM = 1
VIA_TO = 6
VIA_FIRST = 10
VIA_SECOND = 27
BACK = 4
BACK_FROM = 2
BACK_FIRST = 197
BACK_SECOND = 202
BLOCK = 32
PIECES = 1
PAD = 8
KERNEL_VMEM = 57 * 1024 * 1024


def next_z(field, last):
    return jnp.where(last, 0.0, pltpu.roll(field, field.shape[1] - 1, 1))


def prev_z(field, first):
    return jnp.where(first, 0.0, pltpu.roll(field, 1, 1))


def kernel(
    e_in, h_in, labels_in, kpoint_in, eps_inf_in, delta_eps_in, omega_zero_in, damping_in,
    e, h,
    kpoint, eps_inf, delta_eps, omega_zero, damping, load_s,
    p, cur, ce, ja, jb, de, labels, part, sent, ge, ga, phase,
    load_e, load_h, load_l, send_e, recv_e, send_a, recv_a,
    relay, send_r, recv_r, behind_e, send_b, recv_b, ready,
):
    planes, ny, nz = labels.shape
    count = eps_inf.shape[0]
    rows = ny // CHUNKS
    last_plane = planes - 1
    size = lax.axis_size("gx")
    me = lax.axis_index("gx")
    right = lax.rem(me + 1, size)
    relay_one = 2 * size // 3
    relay_two = size // 3 + 1
    back_one, back_two = relay_two - 1, relay_one - 1
    left = lax.rem(me + size - 1, size)

    def span(c, pad=0):
        return pl.ds(pl.multiple_of(c * rows + pad, 8), rows)

    starts = [0] + [k for k in (2, 4, 8, 16, 32) if k < CHUNKS]
    groups = list(zip(starts, starts[1:] + [CHUNKS]))

    def get_e(g):
        low, high = groups[g]
        at = pl.ds(low * rows, (high - low) * rows)
        return pltpu.make_async_copy(
            e_in.at[:, :, :, at], e.at[:, :, :, at], load_e.at[g])

    def get_h(g):
        low, high = groups[g]
        at = pl.ds(low * rows, (high - low) * rows)
        ath = pl.ds(low * rows + PAD, (high - low) * rows)
        return pltpu.make_async_copy(
            h_in.at[:, :, :, at], h.at[:, :, :, ath], load_h.at[g])

    def get_labels():
        return pltpu.make_async_copy(labels_in, labels, load_l)

    def ship_first(c):
        return pltpu.make_async_remote_copy(
            src_ref=e.at[:, 1:3, 0, span(c)], dst_ref=ge.at[0, :, :, span(c)],
            send_sem=send_e.at[0, c], recv_sem=recv_e.at[0, c],
            device_id={"gx": left}, device_id_type=MESH)

    def ship_e(n, c):
        return pltpu.make_async_remote_copy(
            src_ref=sent.at[n % 2, :, :, span(c)], dst_ref=ge.at[n % 2, :, :, span(c)],
            send_sem=send_e.at[n % 2, c], recv_sem=recv_e.at[n % 2, c],
            device_id={"gx": left}, device_id_type=MESH)

    def ship_a(n, c):
        return pltpu.make_async_remote_copy(
            src_ref=part.at[:, :, span(c)], dst_ref=ga.at[n % 2, :, :, span(c)],
            send_sem=send_a.at[c], recv_sem=recv_a.at[n % 2, c],
            device_id={"gx": right}, device_id_type=MESH)

    def ship_via(n, c):
        return pltpu.make_async_remote_copy(
            src_ref=part.at[:, :, span(c)], dst_ref=relay.at[n - VIA_FROM],
            send_sem=send_a.at[c], recv_sem=recv_r.at[n - VIA_FROM],
            device_id={"gx": relay_one}, device_id_type=MESH)

    def pass_on(n):
        return pltpu.make_async_remote_copy(
            src_ref=relay.at[n - VIA_FROM], dst_ref=relay.at[n - VIA_FROM],
            send_sem=send_r.at[n - VIA_FROM], recv_sem=recv_r.at[n - VIA_FROM],
            device_id={"gx": relay_two}, device_id_type=MESH)

    def pass_last(n):
        return pltpu.make_async_remote_copy(
            src_ref=relay.at[n - VIA_FROM], dst_ref=ga.at[n % 2, :, :, span(n % CHUNKS)],
            send_sem=send_r.at[n - VIA_FROM], recv_sem=recv_a.at[n % 2, n % CHUNKS],
            device_id={"gx": 0}, device_id_type=MESH)

    def back_chunk(k):
        return (ITERS - 1 + BACK_FROM + k) % CHUNKS

    def back_ship(k):
        c = back_chunk(k)
        return pltpu.make_async_remote_copy(
            src_ref=sent.at[(ITERS - 1) % 2, :, :, span(c)], dst_ref=behind_e.at[k],
            send_sem=send_e.at[(ITERS - 1) % 2, c], recv_sem=recv_b.at[k],
            device_id={"gx": back_one}, device_id_type=MESH)

    def back_pass(k):
        return pltpu.make_async_remote_copy(
            src_ref=behind_e.at[k], dst_ref=behind_e.at[k],
            send_sem=send_b.at[k], recv_sem=recv_b.at[k],
            device_id={"gx": back_two}, device_id_type=MESH)

    def back_last(k):
        c = back_chunk(k)
        return pltpu.make_async_remote_copy(
            src_ref=behind_e.at[k], dst_ref=ge.at[(ITERS - 1) % 2, :, :, span(c)],
            send_sem=send_b.at[k], recv_sem=recv_e.at[(ITERS - 1) % 2, c],
            device_id={"gx": size - 1}, device_id_type=MESH)

    barrier = pltpu.get_barrier_semaphore()
    for neighbour in (left, right):
        pl.semaphore_signal(barrier, inc=1, device_id={"gx": neighbour}, device_id_type=MESH)
    for target, source in (
        (relay_one, size - 1), (relay_two, relay_one), (0, relay_two),
        (0, back_one), (back_one, back_two), (back_two, size - 1),
    ):
        @pl.when(me == target)
        def _():
            pl.semaphore_signal(barrier, inc=1, device_id={"gx": source}, device_id_type=MESH)
    for g in range(len(groups)):
        get_e(g).start()
        get_h(g).start()
    get_labels().start()
    scalars = [
        pltpu.make_async_copy(source, target, load_s.at[k])
        for k, (source, target) in enumerate((
            (kpoint_in, kpoint), (eps_inf_in, eps_inf), (delta_eps_in, delta_eps),
            (omega_zero_in, omega_zero), (damping_in, damping)))
    ]
    for copy in scalars:
        copy.start()

    shape = (BLOCK, nz)

    def prepare():
        tile = (8, nz)
        turn = jnp.float32(2.0 * math.pi)
        theta_x = turn * jnp.full(tile, kpoint[0], jnp.int32).astype(jnp.float32) / KGRID
        theta_y = turn * jnp.full(tile, kpoint[1], jnp.int32).astype(jnp.float32) / KGRID
        cos_x, sin_x = jnp.cos(theta_x), jnp.sin(theta_x)
        phase[0] = jnp.where(me == size - 1, cos_x, 1.0)
        phase[1] = jnp.where(me == size - 1, sin_x, 0.0)
        phase[2] = jnp.where(me == 0, cos_x, 1.0)
        phase[3] = jnp.where(me == 0, -sin_x, 0.0)
        phase[4] = jnp.cos(theta_y)
        phase[5] = jnp.sin(theta_y)

        def whole(value):
            return jnp.full(tile, value, jnp.float32)

        for label in range(count):
            half = whole(damping[label]) * (DT / 2.0)
            omega = whole(omega_zero[label])
            phase[8 + label] = DT / whole(eps_inf[label])
            phase[8 + count + label] = (1.0 - half) / (1.0 + half)
            phase[8 + 2 * count + label] = DT * omega * omega / (1.0 + half)
            phase[8 + 3 * count + label] = whole(delta_eps[label])

    def spread(row):
        return jnp.concatenate([phase[row]] * (BLOCK // 8), axis=0)

    def media(block, carry):
        at = pl.ds(pl.multiple_of(block * BLOCK, 8), BLOCK)
        zero = jnp.zeros(shape, jnp.float32)
        for x in range(planes):
            label = labels[x, at]
            for which, dst in enumerate((ce, ja, jb, de)):
                picked = spread(8 + count * which)
                for k in range(1, count):
                    picked = jnp.where(label == k, spread(8 + count * which + k), picked)
                dst[x, at] = picked
            for q in range(2):
                for comp in range(3):
                    p[q, comp, x, at] = zero
                    cur[q, comp, x, at] = zero
        return carry

    column = lax.broadcasted_iota(jnp.int32, shape, 1)
    is_first, is_last = column == 0, column == nz - 1

    def wrap_e():
        cy, sy = phase[4][0:1], phase[5][0:1]
        for comp in (0, 2):
            for x in range(planes):
                re, im = e[0, comp, x, 0:1], e[1, comp, x, 0:1]
                e[0, comp, x, ny:ny + 1] = re * cy - im * sy
                e[1, comp, x, ny:ny + 1] = re * sy + im * cy

    def wrap_h():
        cy, sy = phase[4][0:1], phase[5][0:1]
        bottom = PAD + ny - 1
        for comp in (0, 2):
            for x in range(planes):
                re, im = h[0, comp, x, bottom:bottom + 1], h[1, comp, x, bottom:bottom + 1]
                h[0, comp, x, PAD - 1:PAD] = re * cy + im * sy
                h[1, comp, x, PAD - 1:PAD] = im * cy - re * sy

    def turned(ghost, slot, at, row):
        cx, sx = spread(row), spread(row + 1)
        out = []
        for comp in range(2):
            re, im = ghost[slot, 0, comp, at], ghost[slot, 1, comp, at]
            out.append((re * cx - im * sx, re * sx + im * cx))
        return out

    def magnetic(c):
        def block(b, carry):
            y = c * rows + b * BLOCK
            at = pl.ds(pl.multiple_of(y, 8), BLOCK)
            up = pl.ds(y + 1, BLOCK)
            ath = pl.ds(pl.multiple_of(y + PAD, 8), BLOCK)
            for q in range(2):
                for x in range(planes):
                    ex, ey, ez = e[q, 0, x, at], e[q, 1, x, at], e[q, 2, x, at]
                    ex_y, ez_y = e[q, 0, x, up], e[q, 2, x, up]
                    ex_z, ey_z = next_z(ex, is_last), next_z(ey, is_last)
                    h[q, 0, x, ath] -= DT * ((ez_y - ez) - (ey_z - ey))
                    if x == last_plane:
                        hy = h[q, 1, x, ath] - DT * ((ex_z - ex) + ez)
                        hz = h[q, 2, x, ath] + DT * (ey + (ex_y - ex))
                        part[q, 0, at] = hy
                        part[q, 1, at] = hz
                        h[q, 1, x, ath] = hy
                        h[q, 2, x, ath] = hz
                    else:
                        ey_x, ez_x = e[q, 1, x + 1, at], e[q, 2, x + 1, at]
                        h[q, 1, x, ath] -= DT * ((ex_z - ex) - (ez_x - ez))
                        h[q, 2, x, ath] -= DT * ((ey_x - ey) - (ex_y - ex))
            return carry

        lax.fori_loop(0, rows // BLOCK, block, 0)

    def complete(slot, c):
        def block(b, carry):
            y = c * rows + b * BLOCK
            at = pl.ds(pl.multiple_of(y, 8), BLOCK)
            ath = pl.ds(pl.multiple_of(y + PAD, 8), BLOCK)
            far_y, far_z = turned(ge, slot, at, 0)
            for q in range(2):
                h[q, 1, last_plane, ath] += DT * far_z[q]
                h[q, 2, last_plane, ath] -= DT * far_y[q]
            return carry

        lax.fori_loop(0, rows // BLOCK, block, 0)

    def electric(slot, c):
        def block(b, carry):
            y = c * rows + b * BLOCK
            at = pl.ds(pl.multiple_of(y, 8), BLOCK)
            ath = pl.ds(pl.multiple_of(y + PAD, 8), BLOCK)
            down = pl.ds(y + PAD - 1, BLOCK)
            far = turned(ga, slot, at, 2)
            for x in range(planes):
                c_e, j_a, j_b, d_e = ce[x, at], ja[x, at], jb[x, at], de[x, at]
                for q in range(2):
                    fields = [e[q, comp, x, at] for comp in range(3)]
                    hx, hy, hz = h[q, 0, x, ath], h[q, 1, x, ath], h[q, 2, x, ath]
                    if x == 0:
                        hy_x = far[0][q] + DT * fields[2]
                        hz_x = far[1][q] - DT * fields[1]
                    else:
                        hy_x, hz_x = h[q, 1, x - 1, ath], h[q, 2, x - 1, ath]
                    hx_y, hz_y = h[q, 0, x, down], h[q, 2, x, down]
                    hx_z, hy_z = prev_z(hx, is_first), prev_z(hy, is_first)
                    curls = (
                        (hz - hz_y) - (hy - hy_z),
                        (hx - hx_z) - (hz - hz_x),
                        (hy - hy_x) - (hx - hx_y),
                    )
                    for comp, curl in enumerate(curls):
                        field, polar = fields[comp], p[q, comp, x, at]
                        current = j_a * cur[q, comp, x, at] + j_b * (d_e * field - polar)
                        cur[q, comp, x, at] = current
                        p[q, comp, x, at] = polar + DT * current
                        field = field + c_e * (curl - current)
                        e[q, comp, x, at] = field
                        if x == 0 and comp > 0:
                            sent[1 - slot, q, comp - 1, at] = field
            return carry

        lax.fori_loop(0, rows // BLOCK, block, 0)

    total = ITERS * CHUNKS
    relays = (me == relay_one) | (me == relay_two)
    backs = (me == back_one) | (me == back_two)
    three = relays | backs
    four = me == size - 1

    @pl.when(three)
    def _():
        pl.semaphore_wait(barrier, 3)

    @pl.when(four)
    def _():
        pl.semaphore_wait(barrier, 4)

    @pl.when(jnp.logical_not(three | four))
    def _():
        pl.semaphore_wait(barrier, 2)

    for source, target in ((size - 1, back_two), (back_two, back_one), (back_one, 0)):
        @pl.when(me == source)
        def _():
            pl.semaphore_signal(ready, inc=1, device_id={"gx": target}, device_id_type=MESH)

    def advance(step, carry):
        i = step - AHEAD

        @pl.when(i == 0)
        def _():
            for copy in scalars:
                copy.wait()
            prepare()
            wrap_e()
            get_labels().wait()
            lax.fori_loop(0, ny // BLOCK, media, 0)

        @pl.when((i >= 0) & (i < total))
        def _():
            n, j = i // CHUNKS, i % CHUNKS
            c = (n + j) % CHUNKS
            ship_e(n, c).wait_recv()
            complete(n % 2, c)

            @pl.when(c == CHUNKS - 1)
            def _():
                wrap_h()

        @pl.when(i > 0)
        def _():
            n, j = (i - 1) // CHUNKS, (i - 1) % CHUNKS
            c = (n + 1 + j) % CHUNKS
            ship_a(n, c).wait_recv()

            @pl.when(n == 0)
            def _():
                ship_first(c).wait_send()

            @pl.when(n > 1)
            def _():
                ship_e(n - 1, c).wait_send()

            electric(n % 2, c)

            @pl.when(c == 0)
            def _():
                wrap_e()

            back = (me == 0) & (n == ITERS - 2) & (j >= BACK_FROM) & (j < BACK_FROM + BACK)

            @pl.when(back)
            def _():
                @pl.when(j == BACK_FROM)
                def _():
                    pl.semaphore_wait(ready, 1)

                back_ship(j - BACK_FROM).start()

            @pl.when((n < ITERS - 1) & jnp.logical_not(back))
            def _():
                ship_e(n + 1, c).start()

        @pl.when(step < total)
        def _():
            n, j = step // CHUNKS, step % CHUNKS
            c = (n + j) % CHUNKS

            for g, (low, high) in enumerate(groups):
                @pl.when(step == max(low - 1, 0))
                def _():
                    get_e(g).wait()
                    for chunk in range(low, high):
                        ship_first(chunk).start()
                    get_h(g).wait()

            @pl.when(n > 0)
            def _():
                ship_a(n, c).wait_send()

            magnetic(c)
            via = (me == size - 1) & (j == 0) & (n >= VIA_FROM) & (n < VIA_TO)

            @pl.when(via)
            def _():
                ship_via(n, c).start()

            @pl.when(jnp.logical_not(via))
            def _():
                ship_a(n, c).start()

        for back_at, late, send in ((back_one, BACK_FIRST, back_pass), (back_two, BACK_SECOND, back_last)):
            @pl.when((me == back_at) & (step >= late) & (step < late + BACK))
            def _():
                @pl.when(step == late)
                def _():
                    pl.semaphore_wait(ready, 1)

                back_pass(step - late).wait_recv()
                send(step - late).start()

        for relay_at, late, send in ((relay_one, VIA_FIRST, pass_on), (relay_two, VIA_SECOND, pass_last)):
            behind = step - late

            @pl.when((me == relay_at) & (behind >= VIA_FROM * CHUNKS)
                     & (behind < VIA_TO * CHUNKS) & (behind % CHUNKS == 0))
            def _():
                n = behind // CHUNKS
                pass_on(n).wait_recv()
                send(n).start()

        return carry

    lax.fori_loop(0, total + 1 + AHEAD, advance, 0)
    for c in range(CHUNKS):
        ship_a(ITERS - 1, c).wait_send()
        ship_e(ITERS - 1, c).wait_send()

    @pl.when(relays)
    def _():
        for n in range(VIA_FROM, VIA_TO):
            pass_on(n).wait_send()

    @pl.when(backs)
    def _():
        for k in range(BACK):
            back_pass(k).wait_send()


def deliver(e, h, e_out, h_out, sems):
    ny = e_out.shape[3]
    copies = []
    step = ny // PIECES
    for q in range(2):
        for comp in range(3):
            for k in range(PIECES):
                y = k * step
                copies.append(pltpu.make_async_copy(
                    e.at[q, comp, :, y:y + step], e_out.at[q, comp, :, y:y + step],
                    sems.at[0, q, comp, k]))
                copies.append(pltpu.make_async_copy(
                    h.at[q, comp, :, PAD + y:PAD + y + step], h_out.at[q, comp, :, y:y + step],
                    sems.at[1, q, comp, k]))
    for copy in copies:
        copy.start()
    for copy in copies:
        copy.wait()


def shards(e_field, h_field, labels, kpoint, eps_inf, delta_eps, omega_zero, damping):
    planes, ny, nz = labels.shape
    fields = (2, 3, planes)
    anywhere = pl.BlockSpec(memory_space=pltpu.HBM)
    near = pl.BlockSpec(memory_space=pltpu.VMEM)

    def vmem(*shape):
        return pltpu.VMEM(shape, jnp.float32)

    def many(*lead):
        return pltpu.SemaphoreType.DMA(lead + (CHUNKS,))

    e_last, h_last = pl.pallas_call(
        kernel,
        out_shape=(vmem(*fields, ny + PAD, nz), vmem(*fields, ny + PAD, nz)),
        in_specs=[anywhere] * 8,
        out_specs=(near, near),
        scratch_shapes=[
            pltpu.SMEM(kpoint.shape, jnp.int32),
            *(pltpu.SMEM(eps_inf.shape, jnp.float32) for _ in range(4)),
            pltpu.SemaphoreType.DMA((5,)),
            vmem(*fields, ny, nz),
            vmem(*fields, ny, nz),
            vmem(planes, ny, nz),
            vmem(planes, ny, nz),
            vmem(planes, ny, nz),
            vmem(planes, ny, nz),
            pltpu.VMEM((planes, ny, nz), jnp.int32),
            vmem(2, 2, ny, nz),
            vmem(2, 2, 2, ny, nz),
            vmem(2, 2, 2, ny, nz),
            vmem(2, 2, 2, ny, nz),
            vmem(24, 8, nz),
            many(), many(), pltpu.SemaphoreType.DMA,
            many(2), many(2), many(), many(2),
            vmem(VIA_TO - VIA_FROM, 2, 2, ny // CHUNKS, nz),
            pltpu.SemaphoreType.DMA((VIA_TO - VIA_FROM,)),
            pltpu.SemaphoreType.DMA((VIA_TO - VIA_FROM,)),
            vmem(BACK, 2, 2, ny // CHUNKS, nz),
            pltpu.SemaphoreType.DMA((BACK,)),
            pltpu.SemaphoreType.DMA((BACK,)),
            pltpu.SemaphoreType.REGULAR,
        ],
        compiler_params=pltpu.CompilerParams(
            collective_id=0, has_side_effects=True, vmem_limit_bytes=KERNEL_VMEM,
        ),
    )(e_field, h_field, labels, kpoint, eps_inf, delta_eps, omega_zero, damping)
    return pl.pallas_call(
        deliver,
        out_shape=(
            jax.ShapeDtypeStruct(e_field.shape, jnp.float32),
            jax.ShapeDtypeStruct(h_field.shape, jnp.float32),
        ),
        in_specs=[near, near],
        out_specs=(anywhere, anywhere),
        scratch_shapes=[pltpu.SemaphoreType.DMA((2, 2, 3, PIECES))],
        compiler_params=pltpu.CompilerParams(vmem_limit_bytes=1024 * 1024),
    )(e_last, h_last)


def solution(mesh):
    placed = (
        P(None, None, ("kpt", "gx"), None, None),
        P(None, None, ("kpt", "gx"), None, None),
        P(("kpt", "gx"), None, None),
        P("kpt"),
        P(),
        P(),
        P(),
        P(),
    )
    return jax.shard_map(
        shards,
        mesh=mesh,
        in_specs=placed,
        out_specs=(
            P(None, None, ("kpt", "gx"), None, None),
            P(None, None, ("kpt", "gx"), None, None),
        ),
        check_vma=False,
    )
```

```python
import functools
import math

import jax
import jax.numpy as jnp
from jax import lax
from jax.experimental import pallas as pl
from jax.experimental.pallas import tpu as pltpu
from jax.sharding import PartitionSpec as P

MESH = pl.DeviceIdType.MESH
ITERS = 12
KGRID = 16
DT = 0.5
CHUNKS = 16
AHEAD = 14
VIA_FROM = 1
VIA_TO = 8
VIA_FIRST = 10
VIA_SECOND = 27
BLOCK = 32
PIECES = 1
PAD = 8
KERNEL_VMEM = 57 * 1024 * 1024


def next_z(field, last):
    return jnp.where(last, 0.0, pltpu.roll(field, field.shape[1] - 1, 1))


def prev_z(field, first):
    return jnp.where(first, 0.0, pltpu.roll(field, 1, 1))


def kernel(
    e_in, h_in, labels_in, kpoint_in, eps_inf_in, delta_eps_in, omega_zero_in, damping_in,
    e, h,
    kpoint, eps_inf, delta_eps, omega_zero, damping, load_s,
    p, cur, ce, ja, jb, de, labels, part, sent, ge, ga, phase,
    load_e, load_h, load_l, send_e, recv_e, send_a, recv_a,
    relay, send_r, recv_r,
):
    planes, ny, nz = labels.shape
    count = eps_inf.shape[0]
    rows = ny // CHUNKS
    last_plane = planes - 1
    size = lax.axis_size("gx")
    me = lax.axis_index("gx")
    right = lax.rem(me + 1, size)
    relay_one = 2 * size // 3
    relay_two = size // 3 + 1
    left = lax.rem(me + size - 1, size)

    def span(c, pad=0):
        return pl.ds(pl.multiple_of(c * rows + pad, 8), rows)

    starts = [0] + [k for k in (2, 4, 8, 16, 32) if k < CHUNKS]
    groups = list(zip(starts, starts[1:] + [CHUNKS]))

    def get_e(g):
        low, high = groups[g]
        at = pl.ds(low * rows, (high - low) * rows)
        return pltpu.make_async_copy(
            e_in.at[:, :, :, at], e.at[:, :, :, at], load_e.at[g])

    def get_h(g):
        low, high = groups[g]
        at = pl.ds(low * rows, (high - low) * rows)
        ath = pl.ds(low * rows + PAD, (high - low) * rows)
        return pltpu.make_async_copy(
            h_in.at[:, :, :, at], h.at[:, :, :, ath], load_h.at[g])

    def get_labels():
        return pltpu.make_async_copy(labels_in, labels, load_l)

    def ship_first(c):
        return pltpu.make_async_remote_copy(
            src_ref=e.at[:, 1:3, 0, span(c)], dst_ref=ge.at[0, :, :, span(c)],
            send_sem=send_e.at[0, c], recv_sem=recv_e.at[0, c],
            device_id={"gx": left}, device_id_type=MESH)

    def ship_e(n, c):
        return pltpu.make_async_remote_copy(
            src_ref=sent.at[n % 2, :, :, span(c)], dst_ref=ge.at[n % 2, :, :, span(c)],
            send_sem=send_e.at[n % 2, c], recv_sem=recv_e.at[n % 2, c],
            device_id={"gx": left}, device_id_type=MESH)

    def ship_a(n, c):
        return pltpu.make_async_remote_copy(
            src_ref=part.at[:, :, span(c)], dst_ref=ga.at[n % 2, :, :, span(c)],
            send_sem=send_a.at[c], recv_sem=recv_a.at[n % 2, c],
            device_id={"gx": right}, device_id_type=MESH)

    def ship_via(n, c):
        return pltpu.make_async_remote_copy(
            src_ref=part.at[:, :, span(c)], dst_ref=relay.at[n - VIA_FROM],
            send_sem=send_a.at[c], recv_sem=recv_r.at[n - VIA_FROM],
            device_id={"gx": relay_one}, device_id_type=MESH)

    def pass_on(n):
        return pltpu.make_async_remote_copy(
            src_ref=relay.at[n - VIA_FROM], dst_ref=relay.at[n - VIA_FROM],
            send_sem=send_r.at[n - VIA_FROM], recv_sem=recv_r.at[n - VIA_FROM],
            device_id={"gx": relay_two}, device_id_type=MESH)

    def pass_last(n):
        return pltpu.make_async_remote_copy(
            src_ref=relay.at[n - VIA_FROM], dst_ref=ga.at[n % 2, :, :, span(n % CHUNKS)],
            send_sem=send_r.at[n - VIA_FROM], recv_sem=recv_a.at[n % 2, n % CHUNKS],
            device_id={"gx": 0}, device_id_type=MESH)

    barrier = pltpu.get_barrier_semaphore()
    for neighbour in (left, right):
        pl.semaphore_signal(barrier, inc=1, device_id={"gx": neighbour}, device_id_type=MESH)
    for target, source in ((relay_one, size - 1), (relay_two, relay_one), (0, relay_two)):
        @pl.when(me == target)
        def _():
            pl.semaphore_signal(barrier, inc=1, device_id={"gx": source}, device_id_type=MESH)
    for g in range(len(groups)):
        get_e(g).start()
        get_h(g).start()
    get_labels().start()
    scalars = [
        pltpu.make_async_copy(source, target, load_s.at[k])
        for k, (source, target) in enumerate((
            (kpoint_in, kpoint), (eps_inf_in, eps_inf), (delta_eps_in, delta_eps),
            (omega_zero_in, omega_zero), (damping_in, damping)))
    ]
    for copy in scalars:
        copy.start()

    shape = (BLOCK, nz)

    def prepare():
        tile = (8, nz)
        turn = jnp.float32(2.0 * math.pi)
        theta_x = turn * jnp.full(tile, kpoint[0], jnp.int32).astype(jnp.float32) / KGRID
        theta_y = turn * jnp.full(tile, kpoint[1], jnp.int32).astype(jnp.float32) / KGRID
        cos_x, sin_x = jnp.cos(theta_x), jnp.sin(theta_x)
        phase[0] = jnp.where(me == size - 1, cos_x, 1.0)
        phase[1] = jnp.where(me == size - 1, sin_x, 0.0)
        phase[2] = jnp.where(me == 0, cos_x, 1.0)
        phase[3] = jnp.where(me == 0, -sin_x, 0.0)
        phase[4] = jnp.cos(theta_y)
        phase[5] = jnp.sin(theta_y)

        def whole(value):
            return jnp.full(tile, value, jnp.float32)

        for label in range(count):
            half = whole(damping[label]) * (DT / 2.0)
            omega = whole(omega_zero[label])
            phase[8 + label] = DT / whole(eps_inf[label])
            phase[8 + count + label] = (1.0 - half) / (1.0 + half)
            phase[8 + 2 * count + label] = DT * omega * omega / (1.0 + half)
            phase[8 + 3 * count + label] = whole(delta_eps[label])

    def spread(row):
        return jnp.concatenate([phase[row]] * (BLOCK // 8), axis=0)

    def media(block, carry):
        at = pl.ds(pl.multiple_of(block * BLOCK, 8), BLOCK)
        zero = jnp.zeros(shape, jnp.float32)
        for x in range(planes):
            label = labels[x, at]
            for which, dst in enumerate((ce, ja, jb, de)):
                picked = spread(8 + count * which)
                for k in range(1, count):
                    picked = jnp.where(label == k, spread(8 + count * which + k), picked)
                dst[x, at] = picked
            for q in range(2):
                for comp in range(3):
                    p[q, comp, x, at] = zero
                    cur[q, comp, x, at] = zero
        return carry

    column = lax.broadcasted_iota(jnp.int32, shape, 1)
    is_first, is_last = column == 0, column == nz - 1

    def wrap_e():
        cy, sy = phase[4][0:1], phase[5][0:1]
        for comp in (0, 2):
            for x in range(planes):
                re, im = e[0, comp, x, 0:1], e[1, comp, x, 0:1]
                e[0, comp, x, ny:ny + 1] = re * cy - im * sy
                e[1, comp, x, ny:ny + 1] = re * sy + im * cy

    def wrap_h():
        cy, sy = phase[4][0:1], phase[5][0:1]
        bottom = PAD + ny - 1
        for comp in (0, 2):
            for x in range(planes):
                re, im = h[0, comp, x, bottom:bottom + 1], h[1, comp, x, bottom:bottom + 1]
                h[0, comp, x, PAD - 1:PAD] = re * cy + im * sy
                h[1, comp, x, PAD - 1:PAD] = im * cy - re * sy

    def turned(ghost, slot, at, row):
        cx, sx = spread(row), spread(row + 1)
        out = []
        for comp in range(2):
            re, im = ghost[slot, 0, comp, at], ghost[slot, 1, comp, at]
            out.append((re * cx - im * sx, re * sx + im * cx))
        return out

    def magnetic(c):
        def block(b, carry):
            y = c * rows + b * BLOCK
            at = pl.ds(pl.multiple_of(y, 8), BLOCK)
            up = pl.ds(y + 1, BLOCK)
            ath = pl.ds(pl.multiple_of(y + PAD, 8), BLOCK)
            for q in range(2):
                for x in range(planes):
                    ex, ey, ez = e[q, 0, x, at], e[q, 1, x, at], e[q, 2, x, at]
                    ex_y, ez_y = e[q, 0, x, up], e[q, 2, x, up]
                    ex_z, ey_z = next_z(ex, is_last), next_z(ey, is_last)
                    h[q, 0, x, ath] -= DT * ((ez_y - ez) - (ey_z - ey))
                    if x == last_plane:
                        hy = h[q, 1, x, ath] - DT * ((ex_z - ex) + ez)
                        hz = h[q, 2, x, ath] + DT * (ey + (ex_y - ex))
                        part[q, 0, at] = hy
                        part[q, 1, at] = hz
                        h[q, 1, x, ath] = hy
                        h[q, 2, x, ath] = hz
                    else:
                        ey_x, ez_x = e[q, 1, x + 1, at], e[q, 2, x + 1, at]
                        h[q, 1, x, ath] -= DT * ((ex_z - ex) - (ez_x - ez))
                        h[q, 2, x, ath] -= DT * ((ey_x - ey) - (ex_y - ex))
            return carry

        lax.fori_loop(0, rows // BLOCK, block, 0)

    def complete(slot, c):
        def block(b, carry):
            y = c * rows + b * BLOCK
            at = pl.ds(pl.multiple_of(y, 8), BLOCK)
            ath = pl.ds(pl.multiple_of(y + PAD, 8), BLOCK)
            far_y, far_z = turned(ge, slot, at, 0)
            for q in range(2):
                h[q, 1, last_plane, ath] += DT * far_z[q]
                h[q, 2, last_plane, ath] -= DT * far_y[q]
            return carry

        lax.fori_loop(0, rows // BLOCK, block, 0)

    def electric(slot, c):
        def block(b, carry):
            y = c * rows + b * BLOCK
            at = pl.ds(pl.multiple_of(y, 8), BLOCK)
            ath = pl.ds(pl.multiple_of(y + PAD, 8), BLOCK)
            down = pl.ds(y + PAD - 1, BLOCK)
            far = turned(ga, slot, at, 2)
            for x in range(planes):
                c_e, j_a, j_b, d_e = ce[x, at], ja[x, at], jb[x, at], de[x, at]
                for q in range(2):
                    fields = [e[q, comp, x, at] for comp in range(3)]
                    hx, hy, hz = h[q, 0, x, ath], h[q, 1, x, ath], h[q, 2, x, ath]
                    if x == 0:
                        hy_x = far[0][q] + DT * fields[2]
                        hz_x = far[1][q] - DT * fields[1]
                    else:
                        hy_x, hz_x = h[q, 1, x - 1, ath], h[q, 2, x - 1, ath]
                    hx_y, hz_y = h[q, 0, x, down], h[q, 2, x, down]
                    hx_z, hy_z = prev_z(hx, is_first), prev_z(hy, is_first)
                    curls = (
                        (hz - hz_y) - (hy - hy_z),
                        (hx - hx_z) - (hz - hz_x),
                        (hy - hy_x) - (hx - hx_y),
                    )
                    for comp, curl in enumerate(curls):
                        field, polar = fields[comp], p[q, comp, x, at]
                        current = j_a * cur[q, comp, x, at] + j_b * (d_e * field - polar)
                        cur[q, comp, x, at] = current
                        p[q, comp, x, at] = polar + DT * current
                        field = field + c_e * (curl - current)
                        e[q, comp, x, at] = field
                        if x == 0 and comp > 0:
                            sent[1 - slot, q, comp - 1, at] = field
            return carry

        lax.fori_loop(0, rows // BLOCK, block, 0)

    total = ITERS * CHUNKS
    relays = (me == relay_one) | (me == relay_two)
    three = relays | (me == size - 1)

    @pl.when(three)
    def _():
        pl.semaphore_wait(barrier, 3)

    @pl.when(jnp.logical_not(three))
    def _():
        pl.semaphore_wait(barrier, 2)

    def advance(step, carry):
        i = step - AHEAD

        @pl.when(i == 0)
        def _():
            for copy in scalars:
                copy.wait()
            prepare()
            wrap_e()
            get_labels().wait()
            lax.fori_loop(0, ny // BLOCK, media, 0)

        @pl.when((i >= 0) & (i < total))
        def _():
            n, j = i // CHUNKS, i % CHUNKS
            c = (n + j) % CHUNKS
            ship_e(n, c).wait_recv()
            complete(n % 2, c)

            @pl.when(c == CHUNKS - 1)
            def _():
                wrap_h()

        @pl.when(i > 0)
        def _():
            n, j = (i - 1) // CHUNKS, (i - 1) % CHUNKS
            c = (n + 1 + j) % CHUNKS
            ship_a(n, c).wait_recv()

            @pl.when(n == 0)
            def _():
                ship_first(c).wait_send()

            @pl.when(n > 1)
            def _():
                ship_e(n - 1, c).wait_send()

            electric(n % 2, c)

            @pl.when(c == 0)
            def _():
                wrap_e()

            @pl.when(n < ITERS - 1)
            def _():
                ship_e(n + 1, c).start()

        @pl.when(step < total)
        def _():
            n, j = step // CHUNKS, step % CHUNKS
            c = (n + j) % CHUNKS

            for g, (low, high) in enumerate(groups):
                @pl.when(step == max(low - 1, 0))
                def _():
                    get_e(g).wait()
                    for chunk in range(low, high):
                        ship_first(chunk).start()
                    get_h(g).wait()

            @pl.when(n > 0)
            def _():
                ship_a(n, c).wait_send()

            magnetic(c)
            via = (me == size - 1) & (j == 0) & (n >= VIA_FROM) & (n < VIA_TO)

            @pl.when(via)
            def _():
                ship_via(n, c).start()

            @pl.when(jnp.logical_not(via))
            def _():
                ship_a(n, c).start()

        for relay_at, late, send in ((relay_one, VIA_FIRST, pass_on), (relay_two, VIA_SECOND, pass_last)):
            behind = step - late

            @pl.when((me == relay_at) & (behind >= VIA_FROM * CHUNKS)
                     & (behind < VIA_TO * CHUNKS) & (behind % CHUNKS == 0))
            def _():
                n = behind // CHUNKS
                pass_on(n).wait_recv()
                send(n).start()

        return carry

    lax.fori_loop(0, total + 1 + AHEAD, advance, 0)
    for c in range(CHUNKS):
        ship_a(ITERS - 1, c).wait_send()
        ship_e(ITERS - 1, c).wait_send()

    @pl.when(relays)
    def _():
        for n in range(VIA_FROM, VIA_TO):
            pass_on(n).wait_send()


def deliver(e, h, e_out, h_out, sems):
    ny = e_out.shape[3]
    copies = []
    step = ny // PIECES
    for q in range(2):
        for comp in range(3):
            for k in range(PIECES):
                y = k * step
                copies.append(pltpu.make_async_copy(
                    e.at[q, comp, :, y:y + step], e_out.at[q, comp, :, y:y + step],
                    sems.at[0, q, comp, k]))
                copies.append(pltpu.make_async_copy(
                    h.at[q, comp, :, PAD + y:PAD + y + step], h_out.at[q, comp, :, y:y + step],
                    sems.at[1, q, comp, k]))
    for copy in copies:
        copy.start()
    for copy in copies:
        copy.wait()


def shards(e_field, h_field, labels, kpoint, eps_inf, delta_eps, omega_zero, damping):
    planes, ny, nz = labels.shape
    fields = (2, 3, planes)
    anywhere = pl.BlockSpec(memory_space=pltpu.HBM)
    near = pl.BlockSpec(memory_space=pltpu.VMEM)

    def vmem(*shape):
        return pltpu.VMEM(shape, jnp.float32)

    def many(*lead):
        return pltpu.SemaphoreType.DMA(lead + (CHUNKS,))

    e_last, h_last = pl.pallas_call(
        kernel,
        out_shape=(vmem(*fields, ny + PAD, nz), vmem(*fields, ny + PAD, nz)),
        in_specs=[anywhere] * 8,
        out_specs=(near, near),
        scratch_shapes=[
            pltpu.SMEM(kpoint.shape, jnp.int32),
            *(pltpu.SMEM(eps_inf.shape, jnp.float32) for _ in range(4)),
            pltpu.SemaphoreType.DMA((5,)),
            vmem(*fields, ny, nz),
            vmem(*fields, ny, nz),
            vmem(planes, ny, nz),
            vmem(planes, ny, nz),
            vmem(planes, ny, nz),
            vmem(planes, ny, nz),
            pltpu.VMEM((planes, ny, nz), jnp.int32),
            vmem(2, 2, ny, nz),
            vmem(2, 2, 2, ny, nz),
            vmem(2, 2, 2, ny, nz),
            vmem(2, 2, 2, ny, nz),
            vmem(24, 8, nz),
            many(), many(), pltpu.SemaphoreType.DMA,
            many(2), many(2), many(), many(2),
            vmem(VIA_TO - VIA_FROM, 2, 2, ny // CHUNKS, nz),
            pltpu.SemaphoreType.DMA((VIA_TO - VIA_FROM,)),
            pltpu.SemaphoreType.DMA((VIA_TO - VIA_FROM,)),
        ],
        compiler_params=pltpu.CompilerParams(
            collective_id=0, has_side_effects=True, vmem_limit_bytes=KERNEL_VMEM,
        ),
    )(e_field, h_field, labels, kpoint, eps_inf, delta_eps, omega_zero, damping)
    return pl.pallas_call(
        deliver,
        out_shape=(
            jax.ShapeDtypeStruct(e_field.shape, jnp.float32),
            jax.ShapeDtypeStruct(h_field.shape, jnp.float32),
        ),
        in_specs=[near, near],
        out_specs=(anywhere, anywhere),
        scratch_shapes=[pltpu.SemaphoreType.DMA((2, 2, 3, PIECES))],
        compiler_params=pltpu.CompilerParams(vmem_limit_bytes=1024 * 1024),
    )(e_last, h_last)


def solution(mesh):
    placed = (
        P(None, None, ("kpt", "gx"), None, None),
        P(None, None, ("kpt", "gx"), None, None),
        P(("kpt", "gx"), None, None),
        P("kpt"),
        P(),
        P(),
        P(),
        P(),
    )
    return jax.shard_map(
        shards,
        mesh=mesh,
        in_specs=placed,
        out_specs=(
            P(None, None, ("kpt", "gx"), None, None),
            P(None, None, ("kpt", "gx"), None, None),
        ),
        check_vma=False,
    )
```

```python
import functools
import math

import jax
import jax.numpy as jnp
from jax import lax
from jax.experimental import pallas as pl
from jax.experimental.pallas import tpu as pltpu
from jax.sharding import PartitionSpec as P

MESH = pl.DeviceIdType.MESH
ITERS = 12
KGRID = 16
DT = 0.5
CHUNKS = 16
AHEAD = 14
VIA_FROM = 1
VIA_TO = 5
VIA_FIRST = 10
VIA_SECOND = 27
BLOCK = 32
PAD = 8
KERNEL_VMEM = 57 * 1024 * 1024


def next_z(field, last):
    return jnp.where(last, 0.0, pltpu.roll(field, field.shape[1] - 1, 1))


def prev_z(field, first):
    return jnp.where(first, 0.0, pltpu.roll(field, 1, 1))


def kernel(
    e_in, h_in, labels_in, kpoint_in, eps_inf_in, delta_eps_in, omega_zero_in, damping_in,
    e, h,
    kpoint, eps_inf, delta_eps, omega_zero, damping, load_s,
    p, cur, ce, ja, jb, de, labels, part, sent, ge, ga, phase,
    load_e, load_h, load_l, send_e, recv_e, send_a, recv_a,
    relay, send_r, recv_r,
):
    planes, ny, nz = labels.shape
    count = eps_inf.shape[0]
    rows = ny // CHUNKS
    last_plane = planes - 1
    size = lax.axis_size("gx")
    me = lax.axis_index("gx")
    right = lax.rem(me + 1, size)
    relay_one = 2 * size // 3
    relay_two = size // 3 + 1
    left = lax.rem(me + size - 1, size)

    def span(c, pad=0):
        return pl.ds(pl.multiple_of(c * rows + pad, 8), rows)

    starts = [0] + [k for k in (2, 4, 8, 16, 32) if k < CHUNKS]
    groups = list(zip(starts, starts[1:] + [CHUNKS]))

    def get_e(g):
        low, high = groups[g]
        at = pl.ds(low * rows, (high - low) * rows)
        return pltpu.make_async_copy(
            e_in.at[:, :, :, at], e.at[:, :, :, at], load_e.at[g])

    def get_h(g):
        low, high = groups[g]
        at = pl.ds(low * rows, (high - low) * rows)
        ath = pl.ds(low * rows + PAD, (high - low) * rows)
        return pltpu.make_async_copy(
            h_in.at[:, :, :, at], h.at[:, :, :, ath], load_h.at[g])

    def get_labels():
        return pltpu.make_async_copy(labels_in, labels, load_l)

    def ship_first(c):
        return pltpu.make_async_remote_copy(
            src_ref=e.at[:, 1:3, 0, span(c)], dst_ref=ge.at[0, :, :, span(c)],
            send_sem=send_e.at[0, c], recv_sem=recv_e.at[0, c],
            device_id={"gx": left}, device_id_type=MESH)

    def ship_e(n, c):
        return pltpu.make_async_remote_copy(
            src_ref=sent.at[n % 2, :, :, span(c)], dst_ref=ge.at[n % 2, :, :, span(c)],
            send_sem=send_e.at[n % 2, c], recv_sem=recv_e.at[n % 2, c],
            device_id={"gx": left}, device_id_type=MESH)

    def ship_a(n, c):
        return pltpu.make_async_remote_copy(
            src_ref=part.at[:, :, span(c)], dst_ref=ga.at[n % 2, :, :, span(c)],
            send_sem=send_a.at[c], recv_sem=recv_a.at[n % 2, c],
            device_id={"gx": right}, device_id_type=MESH)

    def ship_via(n, c):
        return pltpu.make_async_remote_copy(
            src_ref=part.at[:, :, span(c)], dst_ref=relay.at[n - VIA_FROM],
            send_sem=send_a.at[c], recv_sem=recv_r.at[n - VIA_FROM],
            device_id={"gx": relay_one}, device_id_type=MESH)

    def pass_on(n):
        return pltpu.make_async_remote_copy(
            src_ref=relay.at[n - VIA_FROM], dst_ref=relay.at[n - VIA_FROM],
            send_sem=send_r.at[n - VIA_FROM], recv_sem=recv_r.at[n - VIA_FROM],
            device_id={"gx": relay_two}, device_id_type=MESH)

    def pass_last(n):
        return pltpu.make_async_remote_copy(
            src_ref=relay.at[n - VIA_FROM], dst_ref=ga.at[n % 2, :, :, span(n % CHUNKS)],
            send_sem=send_r.at[n - VIA_FROM], recv_sem=recv_a.at[n % 2, n % CHUNKS],
            device_id={"gx": 0}, device_id_type=MESH)

    barrier = pltpu.get_barrier_semaphore()
    for neighbour in (left, right):
        pl.semaphore_signal(barrier, inc=1, device_id={"gx": neighbour}, device_id_type=MESH)
    for target, source in ((relay_one, size - 1), (relay_two, relay_one), (0, relay_two)):
        @pl.when(me == target)
        def _():
            pl.semaphore_signal(barrier, inc=1, device_id={"gx": source}, device_id_type=MESH)
    for g in range(len(groups)):
        get_e(g).start()
        get_h(g).start()
    get_labels().start()
    scalars = [
        pltpu.make_async_copy(source, target, load_s.at[k])
        for k, (source, target) in enumerate((
            (kpoint_in, kpoint), (eps_inf_in, eps_inf), (delta_eps_in, delta_eps),
            (omega_zero_in, omega_zero), (damping_in, damping)))
    ]
    for copy in scalars:
        copy.start()

    shape = (BLOCK, nz)

    def prepare():
        tile = (8, nz)
        turn = jnp.float32(2.0 * math.pi)
        theta_x = turn * jnp.full(tile, kpoint[0], jnp.int32).astype(jnp.float32) / KGRID
        theta_y = turn * jnp.full(tile, kpoint[1], jnp.int32).astype(jnp.float32) / KGRID
        cos_x, sin_x = jnp.cos(theta_x), jnp.sin(theta_x)
        phase[0] = jnp.where(me == size - 1, cos_x, 1.0)
        phase[1] = jnp.where(me == size - 1, sin_x, 0.0)
        phase[2] = jnp.where(me == 0, cos_x, 1.0)
        phase[3] = jnp.where(me == 0, -sin_x, 0.0)
        phase[4] = jnp.cos(theta_y)
        phase[5] = jnp.sin(theta_y)

        def whole(value):
            return jnp.full(tile, value, jnp.float32)

        for label in range(count):
            half = whole(damping[label]) * (DT / 2.0)
            omega = whole(omega_zero[label])
            phase[8 + label] = DT / whole(eps_inf[label])
            phase[8 + count + label] = (1.0 - half) / (1.0 + half)
            phase[8 + 2 * count + label] = DT * omega * omega / (1.0 + half)
            phase[8 + 3 * count + label] = whole(delta_eps[label])

    def spread(row):
        return jnp.concatenate([phase[row]] * (BLOCK // 8), axis=0)

    def media(block, carry):
        at = pl.ds(pl.multiple_of(block * BLOCK, 8), BLOCK)
        zero = jnp.zeros(shape, jnp.float32)
        for x in range(planes):
            label = labels[x, at]
            for which, dst in enumerate((ce, ja, jb, de)):
                picked = spread(8 + count * which)
                for k in range(1, count):
                    picked = jnp.where(label == k, spread(8 + count * which + k), picked)
                dst[x, at] = picked
            for q in range(2):
                for comp in range(3):
                    p[q, comp, x, at] = zero
                    cur[q, comp, x, at] = zero
        return carry

    column = lax.broadcasted_iota(jnp.int32, shape, 1)
    is_first, is_last = column == 0, column == nz - 1

    def wrap_e():
        cy, sy = phase[4][0:1], phase[5][0:1]
        for comp in (0, 2):
            for x in range(planes):
                re, im = e[0, comp, x, 0:1], e[1, comp, x, 0:1]
                e[0, comp, x, ny:ny + 1] = re * cy - im * sy
                e[1, comp, x, ny:ny + 1] = re * sy + im * cy

    def wrap_h():
        cy, sy = phase[4][0:1], phase[5][0:1]
        bottom = PAD + ny - 1
        for comp in (0, 2):
            for x in range(planes):
                re, im = h[0, comp, x, bottom:bottom + 1], h[1, comp, x, bottom:bottom + 1]
                h[0, comp, x, PAD - 1:PAD] = re * cy + im * sy
                h[1, comp, x, PAD - 1:PAD] = im * cy - re * sy

    def turned(ghost, slot, at, row):
        cx, sx = spread(row), spread(row + 1)
        out = []
        for comp in range(2):
            re, im = ghost[slot, 0, comp, at], ghost[slot, 1, comp, at]
            out.append((re * cx - im * sx, re * sx + im * cx))
        return out

    def magnetic(c):
        def block(b, carry):
            y = c * rows + b * BLOCK
            at = pl.ds(pl.multiple_of(y, 8), BLOCK)
            up = pl.ds(y + 1, BLOCK)
            ath = pl.ds(pl.multiple_of(y + PAD, 8), BLOCK)
            for q in range(2):
                for x in range(planes):
                    ex, ey, ez = e[q, 0, x, at], e[q, 1, x, at], e[q, 2, x, at]
                    ex_y, ez_y = e[q, 0, x, up], e[q, 2, x, up]
                    ex_z, ey_z = next_z(ex, is_last), next_z(ey, is_last)
                    h[q, 0, x, ath] -= DT * ((ez_y - ez) - (ey_z - ey))
                    if x == last_plane:
                        hy = h[q, 1, x, ath] - DT * ((ex_z - ex) + ez)
                        hz = h[q, 2, x, ath] + DT * (ey + (ex_y - ex))
                        part[q, 0, at] = hy
                        part[q, 1, at] = hz
                        h[q, 1, x, ath] = hy
                        h[q, 2, x, ath] = hz
                    else:
                        ey_x, ez_x = e[q, 1, x + 1, at], e[q, 2, x + 1, at]
                        h[q, 1, x, ath] -= DT * ((ex_z - ex) - (ez_x - ez))
                        h[q, 2, x, ath] -= DT * ((ey_x - ey) - (ex_y - ex))
            return carry

        lax.fori_loop(0, rows // BLOCK, block, 0)

    def complete(slot, c):
        def block(b, carry):
            y = c * rows + b * BLOCK
            at = pl.ds(pl.multiple_of(y, 8), BLOCK)
            ath = pl.ds(pl.multiple_of(y + PAD, 8), BLOCK)
            far_y, far_z = turned(ge, slot, at, 0)
            for q in range(2):
                h[q, 1, last_plane, ath] += DT * far_z[q]
                h[q, 2, last_plane, ath] -= DT * far_y[q]
            return carry

        lax.fori_loop(0, rows // BLOCK, block, 0)

    def electric(slot, c):
        def block(b, carry):
            y = c * rows + b * BLOCK
            at = pl.ds(pl.multiple_of(y, 8), BLOCK)
            ath = pl.ds(pl.multiple_of(y + PAD, 8), BLOCK)
            down = pl.ds(y + PAD - 1, BLOCK)
            far = turned(ga, slot, at, 2)
            for x in range(planes):
                c_e, j_a, j_b, d_e = ce[x, at], ja[x, at], jb[x, at], de[x, at]
                for q in range(2):
                    fields = [e[q, comp, x, at] for comp in range(3)]
                    hx, hy, hz = h[q, 0, x, ath], h[q, 1, x, ath], h[q, 2, x, ath]
                    if x == 0:
                        hy_x = far[0][q] + DT * fields[2]
                        hz_x = far[1][q] - DT * fields[1]
                    else:
                        hy_x, hz_x = h[q, 1, x - 1, ath], h[q, 2, x - 1, ath]
                    hx_y, hz_y = h[q, 0, x, down], h[q, 2, x, down]
                    hx_z, hy_z = prev_z(hx, is_first), prev_z(hy, is_first)
                    curls = (
                        (hz - hz_y) - (hy - hy_z),
                        (hx - hx_z) - (hz - hz_x),
                        (hy - hy_x) - (hx - hx_y),
                    )
                    for comp, curl in enumerate(curls):
                        field, polar = fields[comp], p[q, comp, x, at]
                        current = j_a * cur[q, comp, x, at] + j_b * (d_e * field - polar)
                        cur[q, comp, x, at] = current
                        p[q, comp, x, at] = polar + DT * current
                        field = field + c_e * (curl - current)
                        e[q, comp, x, at] = field
                        if x == 0 and comp > 0:
                            sent[1 - slot, q, comp - 1, at] = field
            return carry

        lax.fori_loop(0, rows // BLOCK, block, 0)

    total = ITERS * CHUNKS
    relays = (me == relay_one) | (me == relay_two)
    three = relays | (me == size - 1)

    @pl.when(three)
    def _():
        pl.semaphore_wait(barrier, 3)

    @pl.when(jnp.logical_not(three))
    def _():
        pl.semaphore_wait(barrier, 2)

    def advance(step, carry):
        i = step - AHEAD

        @pl.when(i == 0)
        def _():
            for copy in scalars:
                copy.wait()
            prepare()
            wrap_e()
            get_labels().wait()
            lax.fori_loop(0, ny // BLOCK, media, 0)

        @pl.when((i >= 0) & (i < total))
        def _():
            n, j = i // CHUNKS, i % CHUNKS
            c = (n + j) % CHUNKS
            ship_e(n, c).wait_recv()
            complete(n % 2, c)

            @pl.when(c == CHUNKS - 1)
            def _():
                wrap_h()

        @pl.when(i > 0)
        def _():
            n, j = (i - 1) // CHUNKS, (i - 1) % CHUNKS
            c = (n + 1 + j) % CHUNKS
            ship_a(n, c).wait_recv()

            @pl.when(n == 0)
            def _():
                ship_first(c).wait_send()

            @pl.when(n > 1)
            def _():
                ship_e(n - 1, c).wait_send()

            electric(n % 2, c)

            @pl.when(c == 0)
            def _():
                wrap_e()

            @pl.when(n < ITERS - 1)
            def _():
                ship_e(n + 1, c).start()

        @pl.when(step < total)
        def _():
            n, j = step // CHUNKS, step % CHUNKS
            c = (n + j) % CHUNKS

            for g, (low, high) in enumerate(groups):
                @pl.when(step == max(low - 1, 0))
                def _():
                    get_e(g).wait()
                    for chunk in range(low, high):
                        ship_first(chunk).start()
                    get_h(g).wait()

            @pl.when(n > 0)
            def _():
                ship_a(n, c).wait_send()

            magnetic(c)
            via = (me == size - 1) & (j == 0) & (n >= VIA_FROM) & (n < VIA_TO)

            @pl.when(via)
            def _():
                ship_via(n, c).start()

            @pl.when(jnp.logical_not(via))
            def _():
                ship_a(n, c).start()

        for relay_at, late, send in ((relay_one, VIA_FIRST, pass_on), (relay_two, VIA_SECOND, pass_last)):
            behind = step - late

            @pl.when((me == relay_at) & (behind >= VIA_FROM * CHUNKS)
                     & (behind < VIA_TO * CHUNKS) & (behind % CHUNKS == 0))
            def _():
                n = behind // CHUNKS
                pass_on(n).wait_recv()
                send(n).start()

        return carry

    lax.fori_loop(0, total + 1 + AHEAD, advance, 0)
    for c in range(CHUNKS):
        ship_a(ITERS - 1, c).wait_send()
        ship_e(ITERS - 1, c).wait_send()

    @pl.when(relays)
    def _():
        for n in range(VIA_FROM, VIA_TO):
            pass_on(n).wait_send()


def deliver(e, h, e_out, h_out, sems):
    ny = e_out.shape[3]
    copies = (
        pltpu.make_async_copy(h.at[:, :, :, PAD:PAD + ny], h_out, sems.at[0]),
        pltpu.make_async_copy(e.at[:, :, :, 0:ny], e_out, sems.at[1]),
    )
    for copy in copies:
        copy.start()
    for copy in copies:
        copy.wait()


def shards(e_field, h_field, labels, kpoint, eps_inf, delta_eps, omega_zero, damping):
    planes, ny, nz = labels.shape
    fields = (2, 3, planes)
    anywhere = pl.BlockSpec(memory_space=pltpu.HBM)
    near = pl.BlockSpec(memory_space=pltpu.VMEM)

    def vmem(*shape):
        return pltpu.VMEM(shape, jnp.float32)

    def many(*lead):
        return pltpu.SemaphoreType.DMA(lead + (CHUNKS,))

    e_last, h_last = pl.pallas_call(
        kernel,
        out_shape=(vmem(*fields, ny + PAD, nz), vmem(*fields, ny + PAD, nz)),
        in_specs=[anywhere] * 8,
        out_specs=(near, near),
        scratch_shapes=[
            pltpu.SMEM(kpoint.shape, jnp.int32),
            *(pltpu.SMEM(eps_inf.shape, jnp.float32) for _ in range(4)),
            pltpu.SemaphoreType.DMA((5,)),
            vmem(*fields, ny, nz),
            vmem(*fields, ny, nz),
            vmem(planes, ny, nz),
            vmem(planes, ny, nz),
            vmem(planes, ny, nz),
            vmem(planes, ny, nz),
            pltpu.VMEM((planes, ny, nz), jnp.int32),
            vmem(2, 2, ny, nz),
            vmem(2, 2, 2, ny, nz),
            vmem(2, 2, 2, ny, nz),
            vmem(2, 2, 2, ny, nz),
            vmem(24, 8, nz),
            many(), many(), pltpu.SemaphoreType.DMA,
            many(2), many(2), many(), many(2),
            vmem(VIA_TO - VIA_FROM, 2, 2, ny // CHUNKS, nz),
            pltpu.SemaphoreType.DMA((VIA_TO - VIA_FROM,)),
            pltpu.SemaphoreType.DMA((VIA_TO - VIA_FROM,)),
        ],
        compiler_params=pltpu.CompilerParams(
            collective_id=0, has_side_effects=True, vmem_limit_bytes=KERNEL_VMEM,
        ),
    )(e_field, h_field, labels, kpoint, eps_inf, delta_eps, omega_zero, damping)
    return pl.pallas_call(
        deliver,
        out_shape=(
            jax.ShapeDtypeStruct(e_field.shape, jnp.float32),
            jax.ShapeDtypeStruct(h_field.shape, jnp.float32),
        ),
        in_specs=[near, near],
        out_specs=(anywhere, anywhere),
        scratch_shapes=[pltpu.SemaphoreType.DMA((2,))],
        compiler_params=pltpu.CompilerParams(vmem_limit_bytes=1024 * 1024),
    )(e_last, h_last)


def solution(mesh):
    placed = (
        P(None, None, ("kpt", "gx"), None, None),
        P(None, None, ("kpt", "gx"), None, None),
        P(("kpt", "gx"), None, None),
        P("kpt"),
        P(),
        P(),
        P(),
        P(),
    )
    return jax.shard_map(
        shards,
        mesh=mesh,
        in_specs=placed,
        out_specs=(
            P(None, None, ("kpt", "gx"), None, None),
            P(None, None, ("kpt", "gx"), None, None),
        ),
        check_vma=False,
    )
```
